32 devices in a mesh: gx: 4 (over x, core), gy: 4 (over z), gz: 2 (over y).
Axes of the slice: x: 2, y: 2, z: 4, core: 2. Of those that a mesh axis runs over, the one named last changes fastest.
Arguments:
- particle_fields: float32 [20, 262144], P(None, ('gx', 'gy', 'gz')), may hold values from -4 to 4
- step_length: float32 [262144], P(('gx', 'gy', 'gz')), may hold values from 0.1 to 1
- live_mask: int32 [262144], P(('gx', 'gy', 'gz')), may hold values 0 or 1
- dest_cell: int32 [262144], P(('gx', 'gy', 'gz')), may hold values from 0 to 511
- block_counts: int32 [32, 6], P(('gx', 'gy', 'gz')), may hold values from 0 to 12, as said below
- block_lists: int32 [32, 48], P(('gx', 'gy', 'gz')), may hold values from 0 to 87, as said below
Outputs:
- tile_sums: float32 [20, 16384], P(None, ('gx', 'gy', 'gz'))
The draws below stay inside these ranges and needn't reach their ends.
Inputs may be any that keep to these rules, and one draw needn't show every extreme that they name: `block_counts`: columns are directions in the order x lower, x upper, z lower, z upper, y lower, y upper; a count is at most its section's span (6, 6 or 12) and may be 0; at every section some domain receives full spans from both neighbours. `block_lists`: per domain, 6 entries toward the lower x neighbour, 6 toward the upper, then 2 * 6 for z and 24 for y in the same way; entries are block numbers of the domain's pool at that section. Entries below their direction's count are valid: valid entries of one domain over all sections are distinct, and each names an own block or an appended block that its sender filled. Other entries are arbitrary numbers within the pool.
All inputs are finite; a program needn't handle non-finite values. No bound on the sum of `live_mask` on one device may be relied on, other than what follows from the above.
Results may differ from the reference program's by a relative error of at most 0.0003.
Values sent between devices are 32-bit elements; how exact they have to be, the bound alone decides.
A program may use at most 64 MiB of HBM per device.

```python
import math
import jax
import jax.numpy as jnp

FIELDS = 20
BLOCKS = 64
CELLS = 512
CAP_X = 6
CAP_Z = 6
CAP_Y = 12
LIST_LEN = 48
PARTICLES = 262144
N_GX = 4
N_GY = 4
N_GZ = 2


def plan_migration(key):
    shape_grid = (N_GX, N_GY, N_GZ)
    final_count = BLOCKS + 2 * (CAP_X + CAP_Z + CAP_Y)
    pool_index = jnp.arange(final_count, dtype=jnp.int32)
    eligible = jnp.broadcast_to(pool_index < BLOCKS, shape_grid + (final_count,))
    coords = jnp.meshgrid(jnp.arange(N_GX, dtype=jnp.int32), jnp.arange(N_GY, dtype=jnp.int32), jnp.arange(N_GZ, dtype=jnp.int32), indexing='ij')
    extents_grid = jnp.array(shape_grid, dtype=jnp.int32)
    size_now = BLOCKS
    count_parts = []
    list_parts = []
    for section_index, (axis_place, extent) in enumerate(((0, CAP_X), (2, CAP_Z), (1, CAP_Y))):
        section_key = jax.random.fold_in(key, 101 + section_index)
        count_key, pick_key, filler_key, target_key = jax.random.split(section_key, 4)
        rough_draw = jax.random.randint(count_key, shape_grid + (2,), 0, extent + 1, dtype=jnp.int32)
        number = rough_draw * rough_draw // extent
        target = jax.random.randint(target_key, (3,), 0, extents_grid, dtype=jnp.int32)
        step_unit = (jnp.arange(3) == axis_place).astype(jnp.int32)
        lower_site = (target - step_unit) % extents_grid
        upper_site = (target + step_unit) % extents_grid
        at_lower = (coords[0] == lower_site[0]) & (coords[1] == lower_site[1]) & (coords[2] == lower_site[2])
        at_upper = (coords[0] == upper_site[0]) & (coords[1] == upper_site[1]) & (coords[2] == upper_site[2])
        toward_lower = jnp.where(at_upper, extent, number[..., 0]).astype(jnp.int32)
        toward_upper = jnp.where(at_lower, extent, number[..., 1]).astype(jnp.int32)
        scores = jax.random.randint(pick_key, shape_grid + (final_count,), 0, 1 << 20, dtype=jnp.int32) * final_count + pool_index
        scores = jnp.where(eligible, scores, -1)
        chosen = jnp.argsort(-scores, axis=-1)[..., :2 * extent].astype(jnp.int32)
        position = jnp.arange(2 * extent) % extent
        wanted = jnp.where(jnp.arange(2 * extent) < extent, toward_lower[..., None], toward_upper[..., None])
        usable = position < wanted
        filler = jax.random.randint(filler_key, shape_grid + (2 * extent,), 0, size_now, dtype=jnp.int32)
        list_parts.append(jnp.where(usable, chosen, filler))
        count_parts.append(jnp.stack([toward_lower, toward_upper], axis=-1))
        taken_now = jnp.any((chosen[..., :, None] == pool_index) & usable[..., None], axis=-2)
        from_lower = jnp.roll(toward_upper, 1, axis=axis_place)
        from_upper = jnp.roll(toward_lower, -1, axis=axis_place)
        offset = pool_index - size_now
        landed = (offset >= 0) & (offset < extent) & (offset < from_lower[..., None]) | (offset >= extent) & (offset < 2 * extent) & (offset - extent < from_upper[..., None])
        eligible = eligible & jnp.logical_not(taken_now) | landed
        size_now = size_now + 2 * extent
    counts = jnp.concatenate(count_parts, axis=-1).reshape(N_GX * N_GY * N_GZ, 6)
    entries = jnp.concatenate(list_parts, axis=-1).reshape(N_GX * N_GY * N_GZ, 2 * (CAP_X + CAP_Z + CAP_Y))
    return (counts.astype(jnp.int32), entries.astype(jnp.int32))


def draw_block_counts(key, part):
    return plan_migration(key)[0]


def draw_block_lists(key, part):
    return plan_migration(key)[1]


def set_ends(values, stream_key, low, high):
    dims = values.shape
    place = [jax.random.randint(jax.random.fold_in(stream_key, axis), (), 0, dims[axis]) for axis in range(len(dims))]
    values = values.at[tuple(place)].set(low)
    longest = dims.index(max(dims))
    place[longest] = (place[longest] + 1) % dims[longest]
    return values.at[tuple(place)].set(high)


def levels(stream_key, dims, pieces, least, high):
    loudness, own = 1.0, jax.random.fold_in(stream_key, 6)
    for axis_at, shards_of in pieces:
        steps = jnp.exp(jax.random.uniform(jax.random.fold_in(own, axis_at), (shards_of,), jnp.float32, least / len(pieces), high / len(pieces)))
        loudness = loudness * jnp.repeat(steps, dims[axis_at] // shards_of).reshape([-1 if axis == axis_at else 1 for axis in range(len(dims))])
    return loudness


def centred(rng, shape, deviation, reach, cuts=(), kind=jnp.bfloat16):
    values = jax.random.normal(rng, shape, jnp.float32) * deviation
    if len(cuts) > 0:
        values = levels(rng, shape, cuts, -0.22, 0.18) * values
    return jnp.clip(values, min=-reach, max=reach).astype(kind)


def setup_inputs(seed: int = 0) -> dict:
    arg_keys = jax.random.split(jax.random.key(seed), 7)
    return {
        "particle_fields": centred(arg_keys[0], (FIELDS, PARTICLES), 0.25, 4.0, ((1, 32),), jnp.float32),
        "step_length": jnp.clip(jnp.exp(math.log(1.0) - 2.3025851 * jax.random.uniform(arg_keys[1], (PARTICLES,), jnp.float32) ** levels(arg_keys[1], (PARTICLES,), ((0, 32),), -0.2, 0.2)), 0.1, 1.0),
        "live_mask": set_ends((jax.random.randint(arg_keys[2], (PARTICLES,), 0, 4) < 3).astype(jnp.int32), jax.random.fold_in(arg_keys[2], 1), 0, 1),
        "dest_cell": set_ends(jax.random.randint(arg_keys[3], (PARTICLES,), 0, CELLS), jax.random.fold_in(arg_keys[3], 1), 0, CELLS - 1).astype(jnp.int32),
        "block_counts": draw_block_counts(jax.random.fold_in(arg_keys[6], 71), 0),
        "block_lists": draw_block_lists(jax.random.fold_in(arg_keys[6], 71), 0),
    }


def leave_section(holding, chosen, number, axis_place):
    extent = chosen.shape[-1] // 2
    index_full = jnp.broadcast_to(chosen.astype(jnp.int32)[None, :, :, :, :, None], holding.shape[:4] + (2 * extent, 128))
    picked = jnp.take_along_axis(holding, index_full, axis=4)
    position = jnp.arange(2 * extent) % extent
    wanted = jnp.where(jnp.arange(2 * extent) < extent, number[..., 0:1], number[..., 1:2])
    usable = (position < wanted).astype(jnp.float32)
    outgoing = picked * usable[None, :, :, :, :, None]
    from_lower = jnp.roll(outgoing[:, :, :, :, extent:], 1, axis=axis_place + 1)
    from_upper = jnp.roll(outgoing[:, :, :, :, :extent], -1, axis=axis_place + 1)
    return jnp.concatenate([holding, from_lower, from_upper], axis=4)


def reference(particle_fields, step_length, live_mask, dest_cell, block_counts, block_lists):
    advanced = particle_fields[0:3] + step_length[None, :] * particle_fields[3:6]
    carried = jnp.concatenate([advanced, particle_fields[3:], live_mask.astype(jnp.float32)[None, :], dest_cell.astype(jnp.float32)[None, :]], axis=0)
    row_count = FIELDS + 2
    domain_count = N_GX * N_GY * N_GZ
    holding = carried.reshape(row_count, N_GX, N_GY, N_GZ, BLOCKS, 128)
    number = block_counts.reshape(N_GX, N_GY, N_GZ, 6)
    entries = block_lists.reshape(N_GX, N_GY, N_GZ, LIST_LEN)
    first_end = 2 * CAP_X
    second_end = first_end + 2 * CAP_Z
    holding = leave_section(holding, entries[..., :first_end], number[..., 0:2], 0)
    holding = leave_section(holding, entries[..., first_end:second_end], number[..., 2:4], 2)
    before_count = holding.shape[4]
    holding = leave_section(holding, entries[..., second_end:], number[..., 4:6], 1)
    spans = (CAP_X, CAP_X, CAP_Z, CAP_Z, CAP_Y, CAP_Y)
    limits = [jnp.broadcast_to(number[..., column:column + 1], (N_GX, N_GY, N_GZ, extent)) for column, extent in enumerate(spans)]
    wanted = jnp.concatenate(limits, axis=-1)
    position = jnp.concatenate([jnp.arange(extent) for extent in spans])
    listed = (entries[..., :, None] == jnp.arange(before_count)[None, None, None, None, :]) & (position < wanted)[..., None]
    keep_before = 1.0 - jnp.any(listed, axis=3).astype(jnp.float32)
    keep_block = jnp.concatenate([keep_before, jnp.ones((N_GX, N_GY, N_GZ, holding.shape[4] - before_count), jnp.float32)], axis=-1)
    weights = holding[FIELDS] * keep_block[..., None]
    domain = jnp.arange(domain_count, dtype=jnp.int32).reshape(N_GX, N_GY, N_GZ, 1, 1)
    segment = (domain * CELLS + holding[FIELDS + 1].astype(jnp.int32)).reshape(-1)
    columns = []
    for field_index in range(FIELDS):
        columns.append(jax.ops.segment_sum((holding[field_index] * weights).reshape(-1), segment, num_segments=domain_count * CELLS))
    return jnp.stack(columns, axis=0)
```

```python
import functools

import jax
import jax.numpy as jnp
from jax import lax
from jax.experimental import pallas as pl
from jax.experimental.pallas import tpu as pltpu
from jax.sharding import PartitionSpec as P

CELLS = 512
CAP_X = 6
CAP_Z = 6
CAP_Y = 12
LANES = 128
HALF = 256
GROUP = 8
GONE = 8 * CELLS
CLASSES = 3


def migrate_kernel(
    sizes,
    counts_hbm,
    lists_hbm,
    fields_hbm,
    step_hbm,
    live_hbm,
    cell_hbm,
    out_ref,
    fields,
    step,
    live,
    cell,
    pool,
    offsets,
    acc,
    sent_x,
    sent_z,
    got_x,
    got_z,
    sent_y,
    got_y,
    counts,
    lists,
    lists_row,
    load_sem,
    send_sem,
    recv_sem,
):
    field_count = fields_hbm.shape[0]
    rows = pool.shape[1]
    whole = field_count // 8 * 8
    tail = field_count - whole
    blocks = step.shape[0]

    me = {axis: lax.axis_index(axis) for axis in ("gx", "gy", "gz")}
    lower = {axis: {axis: lax.rem(me[axis] + sizes[axis] - 1, sizes[axis])} for axis in me}
    upper = {axis: {axis: lax.rem(me[axis] + 1, sizes[axis])} for axis in me}

    small = [
        pltpu.make_async_copy(counts_hbm, counts, load_sem.at[4]),
        pltpu.make_async_copy(lists_hbm, lists, load_sem.at[5]),
        pltpu.make_async_copy(lists_hbm, lists_row, load_sem.at[6]),
    ]
    loads = [
        pltpu.make_async_copy(fields_hbm, fields, load_sem.at[0]),
        pltpu.make_async_copy(step_hbm, step, load_sem.at[1]),
        pltpu.make_async_copy(live_hbm, live, load_sem.at[2]),
        pltpu.make_async_copy(cell_hbm, cell, load_sem.at[3]),
    ]
    for load in loads + small:
        load.start()

    barrier = pltpu.get_barrier_semaphore()
    for axis in me:
        for neighbour in (lower[axis], upper[axis]):
            pl.semaphore_signal(
                barrier, inc=1, device_id=neighbour, device_id_type=pl.DeviceIdType.MESH
            )

    for load in small:
        load.wait()
    spans = (CAP_X, CAP_X, CAP_Z, CAP_Z, CAP_Y, CAP_Y)
    lane = lax.broadcasted_iota(jnp.int32, lists_row.shape, 1)
    limit = jnp.zeros(lists_row.shape, jnp.int32)
    away = jnp.zeros(lists_row.shape, jnp.float32)
    start = 0
    for k, span in enumerate(spans):
        here = lane >= start
        limit = jnp.where(here, counts[0, k] + start, limit)
        away = jnp.where(here, float(GONE if k < 4 else (k - 3) * CELLS), away)
        start += span
    away = jnp.where(lane < limit, away, 0.0)
    number = lax.broadcasted_iota(jnp.int32, (offsets.shape[0], lists_row.shape[1]), 0)
    named = jnp.where(lists_row[...] == number, away, 0.0)
    offsets[...] = jnp.broadcast_to(jnp.sum(named, axis=1, keepdims=True), offsets.shape)

    for load in loads:
        load.wait()

    first_row = lax.broadcasted_iota(jnp.int32, (8, LANES), 0)

    def own_block(e):
        v = fields[:, pl.ds(pl.multiple_of(e * LANES, LANES), LANES)]
        top = v[:8]
        pace = step[pl.ds(e, 1), :]
        top = top + jnp.where(first_row < 3, pace * pltpu.roll(top, 5, 0), 0.0)
        v = jnp.concatenate([top, v[8:]], axis=0)
        v = v * live[pl.ds(e, 1), :].astype(jnp.float32)
        where_to = cell[pl.ds(e, 1), :].astype(jnp.float32)
        return jnp.concatenate(
            [v, jnp.broadcast_to(where_to, (rows - field_count, LANES))], axis=0
        )

    def exchange(axis, index, sent, got, width):
        out = []
        for side, (target, other) in enumerate(((lower, 1), (upper, 0))):
            copy = pltpu.make_async_remote_copy(
                src_ref=sent.at[pl.ds(side * width, width)],
                dst_ref=got.at[pl.ds(other * width, width)],
                send_sem=send_sem.at[index + side],
                recv_sem=recv_sem.at[index + other],
                device_id=target[axis],
                device_id_type=pl.DeviceIdType.MESH,
            )
            copy.start()
            out.append(copy)
        return out

    def fill(sent, slot, span, first_entry, first_count):
        count = jnp.full((rows, LANES), counts[0, first_count + slot // span])
        block = pool[lists[0, first_entry + slot]]
        block = jnp.where(count > slot % span, block, 0.0)
        side, i = slot // span, slot % span
        sent[side, pl.ds(i * whole, whole), :] = block[:whole]
        tail_at = span * whole + i * tail
        sent[side, pl.ds(tail_at, tail), :] = block[whole:field_count]
        sent[side, pl.ds(span * field_count + i, 1), :] = block[field_count : field_count + 1]

    def unpacked(got, slot, span):
        side, i = slot // span, slot % span
        body = got[side, pl.ds(i * whole, whole), :]
        rest = got[side, pl.ds(span * whole + i * tail, tail), :]
        cells = got[side, pl.ds(span * field_count + i, 1), :]
        spare = jnp.broadcast_to(cells, (rows - field_count, LANES))
        return jnp.concatenate([body, rest, spare], axis=0), cells

    def advance(g, carry):
        for i in range(GROUP):
            pool[g * GROUP + i] = own_block(g * GROUP + i)
        return carry

    lax.fori_loop(0, blocks // GROUP, advance, 0)
    for slot in range(2 * CAP_X):
        fill(sent_x, slot, CAP_X, 0, 0)
    pl.semaphore_wait(barrier, 6)
    copies_x = exchange("gx", 0, sent_x, got_x, 1)

    code = lax.broadcasted_iota(jnp.int32, (HALF, LANES), 0).astype(jnp.float32)
    parts = CLASSES * CELLS // HALF

    def operands(v, cells, wanted=tuple(range(parts))):
        high = v.astype(jnp.bfloat16).astype(jnp.float32)
        both = jnp.concatenate([high, v - high], axis=0)
        part = jnp.floor(cells * (1.0 / HALF))
        inner = cells - part * HALF
        left = jnp.concatenate(
            [jnp.where(part == float(h), both, 0.0).astype(jnp.bfloat16) for h in wanted],
            axis=0,
        )
        right = jnp.where(code == inner, 1.0, 0.0).astype(jnp.bfloat16)
        return left, right

    def bin_group(pairs):
        left = jnp.concatenate([a for a, _ in pairs], axis=1)
        right = jnp.concatenate([b for _, b in pairs], axis=1)
        acc[...] += lax.dot_general(
            left, right, (((1,), (1,)), ((), ())), preferred_element_type=jnp.float32
        )

    acc[...] = jnp.zeros_like(acc)

    def bin_own(g, carry):
        pairs = []
        for i in range(GROUP):
            b = g * GROUP + i
            cells = pool[b, pl.ds(field_count, 1), :] + offsets[pl.ds(b, 1), :]
            pairs.append(operands(pool[b], cells))
        bin_group(pairs)
        return carry

    early = 3 * (blocks // GROUP) // 8
    lax.fori_loop(0, early, bin_own, 0)

    def bin_got(got, side, width, base, wanted=tuple(range(parts))):
        pairs = []
        for i in range(side * width, (side + 1) * width):
            v, cells = unpacked(got, i, width)
            pairs.append(operands(v, cells + offsets[pl.ds(base + i, 1), :], wanted))
        left = jnp.concatenate([a for a, _ in pairs], axis=1)
        right = jnp.concatenate([b for _, b in pairs], axis=1)
        acc[pl.ds(2 * rows * wanted[0], 2 * rows * len(wanted)), :] += lax.dot_general(
            left, right, (((1,), (1,)), ((), ())), preferred_element_type=jnp.float32
        )

    for copy in copies_x:
        copy.wait_recv()
    for slot in range(2 * CAP_X):
        pool[blocks + slot] = unpacked(got_x, slot, CAP_X)[0]
    for slot in range(2 * CAP_Z):
        fill(sent_z, slot, CAP_Z, 2 * CAP_X, 2)
    copies_z = exchange("gz", 2, sent_z, got_z, 1)
    lax.fori_loop(early, blocks // GROUP, bin_own, 0)
    bin_got(got_x, 0, CAP_X, blocks)
    bin_got(got_x, 1, CAP_X, blocks)

    kept_parts = tuple(range(CELLS // HALF))
    bound_parts = tuple(range(CELLS // HALF, parts))
    late = blocks + 2 * CAP_X
    for side in (1, 0):
        pltpu.make_async_remote_copy(
            src_ref=sent_z.at[pl.ds(1 - side, 1)],
            dst_ref=got_z.at[pl.ds(side, 1)],
            send_sem=send_sem.at[3 - side],
            recv_sem=recv_sem.at[2 + side],
            device_id=upper["gz"] if side == 0 else lower["gz"],
            device_id_type=pl.DeviceIdType.MESH,
        ).wait_recv()
        if side == 1:
            bin_got(got_z, side, CAP_Z, late)
        else:
            bin_got(got_z, side, CAP_Z, late, bound_parts)

    def bin_kept(base):
        bin_got(got_z, 0, CAP_Z, base, kept_parts)

    def halves(kind):
        tops = [2 * rows * h for h in range(kind * CELLS // HALF, (kind + 1) * CELLS // HALF)]
        return [
            (acc[pl.ds(t, rows), :] + acc[pl.ds(t + rows, rows), :])[:field_count] for t in tops
        ]

    for side in (0, 1):
        for i, half in enumerate(halves(side + 1)):
            sent_y[side, pl.ds(i * field_count, field_count), :] = half
    copies_y = exchange("gy", 4, sent_y, got_y, 1)
    bin_kept(late)
    kept = halves(0)
    for copy in copies_y:
        copy.wait_recv()
    for i, half in enumerate(kept):
        part = pl.ds(i * field_count, field_count)
        out_ref[:, pl.ds(i * HALF, HALF)] = half + got_y[0, part, :] + got_y[1, part, :]
    for copy in copies_x + copies_z + copies_y:
        copy.wait_send()


def solution(mesh):
    sizes = {axis: mesh.shape[axis] for axis in ("gx", "gy", "gz")}

    def per_device(particle_fields, step_length, live_mask, dest_cell, block_counts, block_lists):
        field_count, particles = particle_fields.shape
        blocks = particles // LANES
        rows = (field_count + 1 + 7) // 8 * 8
        sum_rows = (field_count * CELLS // HALF + 7) // 8 * 8
        pool_blocks = blocks + 2 * CAP_X + 2 * CAP_Z

        def packed(span):
            return (span * (field_count + 1) + 7) // 8 * 8

        by_block = [a.reshape(blocks, LANES) for a in (step_length, live_mask, dest_cell)]
        any_space = pl.BlockSpec(memory_space=pl.ANY)
        vmem = pl.BlockSpec(memory_space=pltpu.VMEM)
        smem = pl.BlockSpec(memory_space=pltpu.SMEM)
        f32 = jnp.float32
        return pl.pallas_call(
            functools.partial(migrate_kernel, sizes),
            out_shape=pltpu.VMEM((field_count, CELLS), f32),
            in_specs=[any_space] * 6,
            out_specs=vmem,
            scratch_shapes=[
                pltpu.VMEM((field_count, particles), f32),
                pltpu.VMEM((blocks, LANES), f32),
                pltpu.VMEM((blocks, LANES), jnp.int32),
                pltpu.VMEM((blocks, LANES), jnp.int32),
                pltpu.VMEM((blocks + 2 * CAP_X, rows, LANES), f32),
                pltpu.VMEM((pool_blocks, LANES), f32),
                pltpu.VMEM((2 * rows * CLASSES * CELLS // HALF, HALF), f32),
                pltpu.VMEM((2, packed(CAP_X), LANES), f32),
                pltpu.VMEM((2, packed(CAP_Z), LANES), f32),
                pltpu.VMEM((2, packed(CAP_X), LANES), f32),
                pltpu.VMEM((2, packed(CAP_Z), LANES), f32),
                pltpu.VMEM((2, sum_rows, HALF), f32),
                pltpu.VMEM((2, sum_rows, HALF), f32),
                pltpu.SMEM(block_counts.shape, jnp.int32),
                pltpu.SMEM(block_lists.shape, jnp.int32),
                pltpu.VMEM(block_lists.shape, jnp.int32),
                pltpu.SemaphoreType.DMA((7,)),
                pltpu.SemaphoreType.DMA((6,)),
                pltpu.SemaphoreType.DMA((6,)),
            ],
            compiler_params=pltpu.CompilerParams(collective_id=0, has_side_effects=True),
        )(block_counts, block_lists, particle_fields, *by_block)

    placed = (
        P(None, ("gx", "gy", "gz")),
        P(("gx", "gy", "gz")),
        P(("gx", "gy", "gz")),
        P(("gx", "gy", "gz")),
        P(("gx", "gy", "gz"), None),
        P(("gx", "gy", "gz"), None),
    )
    return jax.shard_map(
        per_device,
        mesh=mesh,
        in_specs=placed,
        out_specs=P(None, ("gx", "gy", "gz")),
        check_vma=False,
    )
```

```python
import functools

import jax
import jax.numpy as jnp
from jax import lax
from jax.experimental import pallas as pl
from jax.experimental.pallas import tpu as pltpu
from jax.sharding import PartitionSpec as P

CELLS = 512
CAP_X = 6
CAP_Z = 6
CAP_Y = 12
LANES = 128
HALF = 256
GROUP = 8
GONE = 16 * CELLS
AXES = ("gx", "gy", "gz")


def plan(sizes):
    steps_z = (1,) if sizes["gz"] == 2 else (-1, 1)
    classes = [{}, {"gy": -1}, {"gy": 1}]
    for dz in steps_z:
        classes += [{"gz": dz}, {"gz": dz, "gy": -1}, {"gz": dz, "gy": 1}]
    return steps_z, classes


def migrate_kernel(
    sizes,
    counts_hbm,
    lists_hbm,
    fields_hbm,
    step_hbm,
    live_hbm,
    cell_hbm,
    out_ref,
    fields,
    step,
    live,
    cell,
    offsets,
    offsets_x,
    offsets_slot,
    acc_kept,
    acc,
    sent_x,
    got_x,
    sent_meta,
    got_meta,
    sent,
    got,
    counts,
    lists,
    lists_row,
    load_sem,
    send_x_sem,
    recv_x_sem,
    send_meta_sem,
    recv_meta_sem,
    send_sem,
    recv_sem,
):
    steps_z, classes = plan(sizes)
    field_count = fields_hbm.shape[0]
    rows = (field_count + 1 + 7) // 8 * 8
    whole = field_count // 8 * 8
    tail = field_count - whole
    blocks = step.shape[0]
    halves = CELLS // HALF
    start_z, start_y = 2 * CAP_X, 2 * CAP_X + 2 * CAP_Z

    me = {axis: lax.axis_index(axis) for axis in AXES}

    def target(moves):
        return {a: lax.rem(me[a] + sizes[a] + d, sizes[a]) for a, d in moves.items()}

    def remote(src, dst, send, recv, moves):
        return pltpu.make_async_remote_copy(
            src_ref=src,
            dst_ref=dst,
            send_sem=send,
            recv_sem=recv,
            device_id=target(moves),
            device_id_type=pl.DeviceIdType.MESH,
        )

    loads = [
        pltpu.make_async_copy(src, dst, load_sem.at[i])
        for i, (src, dst) in enumerate(
            [
                (counts_hbm, counts),
                (lists_hbm, lists),
                (lists_hbm, lists_row),
                (step_hbm, step),
                (live_hbm, live),
                (cell_hbm, cell),
                (fields_hbm, fields),
            ]
        )
    ]
    for load in loads:
        load.start()

    moves_x = ({"gx": -1}, {"gx": 1})
    partners = {}
    for moves in list(moves_x) + classes[1:]:
        partners[tuple(moves.get(a, 0) % sizes[a] for a in AXES)] = moves
    barrier = pltpu.get_barrier_semaphore()
    for moves in partners.values():
        pl.semaphore_signal(
            barrier, inc=1, device_id=target(moves), device_id_type=pl.DeviceIdType.MESH
        )

    for load in loads:
        load.wait()

    first_row = lax.broadcasted_iota(jnp.int32, (8, LANES), 0)

    def own_block(e):
        v = fields[:, pl.ds(e * LANES, LANES)]
        top = v[:8]
        pace = step[pl.ds(e, 1), :]
        top = top + jnp.where(first_row < 3, pace * pltpu.roll(top, 5, 0), 0.0)
        v = jnp.concatenate([top, v[8:]], axis=0)
        v = v * live[pl.ds(e, 1), :].astype(jnp.float32)
        where_to = cell[pl.ds(e, 1), :].astype(jnp.float32)
        spare = jnp.broadcast_to(where_to, (rows - field_count, LANES))
        return jnp.concatenate([v, spare], axis=0), where_to

    for slot in range(2 * CAP_X):
        block, _ = own_block(jnp.minimum(lists[0, slot], blocks - 1))
        side, i = slot // CAP_X, slot % CAP_X
        count = jnp.full((rows, LANES), counts[0, side])
        block = jnp.where(count > i, block, 0.0)
        sent_x[side, pl.ds(i * whole, whole), :] = block[:whole]
        sent_x[side, pl.ds(CAP_X * whole + i * tail, tail), :] = block[whole:field_count]
        sent_x[side, pl.ds(CAP_X * field_count + i, 1), :] = block[field_count : field_count + 1]

    pl.semaphore_wait(barrier, len(partners))

    def copy_x(side):
        return [
            remote(
                sent_x.at[pl.ds(s, 1)],
                got_x.at[pl.ds(s, 1)],
                send_x_sem.at[s],
                recv_x_sem.at[s],
                moves_x[s],
            )
            for s in side
        ]

    copies_x = copy_x((0, 1))
    for copy in copies_x:
        copy.start()

    lane = lax.broadcasted_iota(jnp.int32, lists_row.shape, 1)
    z_number = blocks + 2 * CAP_X + jnp.where(
        lane < start_z + CAP_Z, lane - start_z + CAP_Z, lane - start_z - CAP_Z
    )
    onward = jnp.zeros(lists_row.shape, jnp.float32)
    for k in range(2 * CAP_Y):
        side, i = k // CAP_Y, k % CAP_Y
        count = jnp.full(lists_row.shape, counts[0, 4 + side])
        hit = (z_number == lists[0, start_y + k]) & (count > i)
        onward = jnp.where(hit, float(1 + side), onward)
    sent_meta[...] = jnp.broadcast_to(onward, sent_meta.shape)
    copies_meta = [
        remote(
            sent_meta, got_meta.at[i], send_meta_sem.at[i], recv_meta_sem.at[i], {"gz": dz}
        )
        for i, dz in enumerate(steps_z)
    ]
    for copy in copies_meta:
        copy.start()

    spans = (CAP_X, CAP_X, CAP_Z, CAP_Z, CAP_Y, CAP_Y)
    limit = jnp.zeros(lists_row.shape, jnp.int32)
    away = jnp.zeros(lists_row.shape, jnp.float32)
    start = 0
    for k, span in enumerate(spans):
        here = lane >= start
        limit = jnp.where(here, counts[0, k] + start, limit)
        away = jnp.where(here, float(GONE if k < 4 else (k - 3) * CELLS), away)
        start += span
    valid = lane < limit
    entries = lists_row[...]
    own_entry = valid & (entries < blocks)

    def table(ref, first, value, by_lane):
        number = first + lax.broadcasted_iota(jnp.int32, (ref.shape[0], lists_row.shape[1]), 0)
        hit = (lane if by_lane else entries) == number
        total = jnp.sum(jnp.where(hit, value, 0.0), axis=1, keepdims=True)
        ref[...] = jnp.broadcast_to(total, ref.shape)

    table(offsets, 0, jnp.where(valid, away, 0.0), False)
    y_slots = offsets_slot.at[pl.ds(2 * CAP_Z, 2 * CAP_Y)]
    table(y_slots, start_y, jnp.where(own_entry, away, float(GONE)), True)

    code = lax.broadcasted_iota(jnp.int32, (HALF, LANES), 0).astype(jnp.float32)

    def operands(v, cells, wanted):
        high = v.astype(jnp.bfloat16).astype(jnp.float32)
        both = jnp.concatenate([high, v - high], axis=0)
        part = jnp.floor(cells * (1.0 / HALF))
        inner = cells - part * HALF
        left = [
            jnp.concatenate(
                [
                    jnp.where(part == float(c * halves + h), both, 0.0).astype(jnp.bfloat16)
                    for c in group
                    for h in range(halves)
                ],
                axis=0,
            )
            for group in wanted
        ]
        right = jnp.where(code == inner, 1.0, 0.0).astype(jnp.bfloat16)
        return left, right

    def span_of(group):
        return pl.ds((group[0] - 1) * halves * 2 * rows, len(group) * halves * 2 * rows)

    def product(pairs, g):
        left = jnp.concatenate([a[g] for a, _ in pairs], axis=1)
        right = jnp.concatenate([b for _, b in pairs], axis=1)
        return lax.dot_general(
            left, right, (((1,), (1,)), ((), ())), preferred_element_type=jnp.float32
        )

    def own_slot(k, group):
        v, cells = own_block(jnp.minimum(lists[0, start_z + k], blocks - 1))
        return operands(v, cells + offsets_slot[pl.ds(k, 1), :], (group,))

    for side in range(2):
        first = 2 * CAP_Z + side * CAP_Y
        pairs = [own_slot(first + i, (1 + side,)) for i in range(CAP_Y)]
        acc[span_of((1 + side,)), :] = product(pairs, 0)

    for copy in copies_meta:
        copy.wait_recv()
    if len(steps_z) == 1:
        kind = got_meta[0, :1, :]
    else:
        kind = jnp.where(lane < start_z + CAP_Z, got_meta[1, :1, :], got_meta[0, :1, :] + 3.0)
    in_z = (lane >= start_z) & (lane < start_y)
    away = jnp.where(in_z, (kind + 3.0) * CELLS, away)
    table(offsets_x, blocks, jnp.where(valid, away, 0.0), False)
    z_slots = offsets_slot.at[pl.ds(0, 2 * CAP_Z)]
    table(z_slots, start_z, jnp.where(own_entry, away, float(GONE)), True)

    z_classes = tuple(range(3, len(classes)))
    pairs = [own_slot(i, z_classes) for i in range(2 * CAP_Z)]
    acc[span_of(z_classes), :] = product(pairs, 0)

    def unpacked(side, i):
        body = got_x[side, pl.ds(i * whole, whole), :]
        rest = got_x[side, pl.ds(CAP_X * whole + i * tail, tail), :]
        cells = got_x[side, pl.ds(CAP_X * field_count + i, 1), :]
        spare = jnp.broadcast_to(cells, (rows - field_count, LANES))
        return jnp.concatenate([body, rest, spare], axis=0), cells

    def got_blocks(side, wanted):
        base = (1 - side) * CAP_X
        pairs = []
        for i in range(CAP_X):
            v, cells = unpacked(side, i)
            pairs.append(operands(v, cells + offsets_x[pl.ds(base + i, 1), :], wanted))
        return pairs

    def wait_x(side):
        pltpu.make_async_remote_copy(
            src_ref=sent_x.at[pl.ds(side, 1)],
            dst_ref=got_x.at[pl.ds(side, 1)],
            send_sem=send_x_sem.at[side],
            recv_sem=recv_x_sem.at[side],
            device_id=target(moves_x[0]),
            device_id_type=pl.DeviceIdType.MESH,
        ).wait_recv()

    near = lax.rem(me["gx"], 2)
    wait_x(near)
    bound = tuple(range(1, len(classes)))
    acc[...] += product(got_blocks(near, (bound,)), 0)

    far = 1 - near
    wait_x(far)
    order = [c for c in bound if len(classes[c]) == 2]
    order += [c for c in bound if list(classes[c]) == ["gy"]]
    order += [c for c in bound if list(classes[c]) == ["gz"]]
    pairs = got_blocks(far, tuple((c,) for c in order))

    def packed(read):
        sums = [read(h, 0) + read(h, 1) for h in range(halves)]
        return [s[:whole] for s in sums] + [s[whole:field_count] for s in sums]

    def store(ref, c, pieces):
        for h in range(halves):
            ref[c, pl.ds(h * whole, whole), :] = pieces[h]
            ref[c, pl.ds(halves * whole + h * tail, tail), :] = pieces[halves + h]

    copies = {}
    for g, c in enumerate(order):
        total = acc[span_of((c,)), :] + product(pairs, g)

        def read(h, k):
            top = (h * 2 + k) * rows
            return total[top : top + rows]

        store(sent, c - 1, packed(read))
        copies[c] = remote(
            sent.at[c - 1],
            got.at[c - 1],
            send_sem.at[c - 1],
            recv_sem.at[c - 1],
            classes[c],
        )
        copies[c].start()

    acc_kept[...] = jnp.zeros_like(acc_kept)
    for side in range(2):
        base = (1 - side) * CAP_X
        pairs = []
        for i in range(CAP_X):
            v, cells = unpacked(side, i)
            pairs.append(operands(v, cells + offsets_x[pl.ds(base + i, 1), :], ((0,),)))
        acc_kept[...] += product(pairs, 0)

    def bin_own(g, carry):
        pairs = []
        for i in range(GROUP):
            b = g * GROUP + i
            v, cells = own_block(b)
            pairs.append(operands(v, cells + offsets[pl.ds(b, 1), :], ((0,),)))
        acc_kept[...] += product(pairs, 0)
        return carry

    lax.fori_loop(0, blocks // GROUP, bin_own, 0)

    total = packed(lambda h, k: acc_kept[pl.ds((h * 2 + k) * rows, rows), :])
    for c in [c for c in order if len(classes[c]) == 1] + [
        c for c in order if len(classes[c]) == 2
    ]:
        copies[c].wait_recv()
        for h in range(halves):
            total[h] = total[h] + got[c - 1, pl.ds(h * whole, whole), :]
            more = got[c - 1, pl.ds(halves * whole + h * tail, tail), :]
            total[halves + h] = total[halves + h] + more
    for h in range(halves):
        out_ref[:whole, pl.ds(h * HALF, HALF)] = total[h]
        out_ref[whole:, pl.ds(h * HALF, HALF)] = total[halves + h]
    for copy in copies_x + copies_meta + list(copies.values()):
        copy.wait_send()


def solution(mesh):
    sizes = {axis: mesh.shape[axis] for axis in AXES}

    def per_device(particle_fields, step_length, live_mask, dest_cell, block_counts, block_lists):
        field_count, particles = particle_fields.shape
        blocks = particles // LANES
        rows = (field_count + 1 + 7) // 8 * 8
        steps_z, classes = plan(sizes)
        sends = len(classes) - 1
        halves = CELLS // HALF
        sum_rows = (field_count * halves + 7) // 8 * 8
        packed_x = (CAP_X * (field_count + 1) + 7) // 8 * 8
        slots = 2 * CAP_Z + 2 * CAP_Y

        by_block = [a.reshape(blocks, LANES) for a in (step_length, live_mask, dest_cell)]
        any_space = pl.BlockSpec(memory_space=pl.ANY)
        f32 = jnp.float32
        return pl.pallas_call(
            functools.partial(migrate_kernel, sizes),
            out_shape=pltpu.VMEM((field_count, CELLS), f32),
            in_specs=[any_space] * 6,
            out_specs=pl.BlockSpec(memory_space=pltpu.VMEM),
            scratch_shapes=[
                pltpu.VMEM((field_count, particles), f32),
                pltpu.VMEM((blocks, LANES), f32),
                pltpu.VMEM((blocks, LANES), jnp.int32),
                pltpu.VMEM((blocks, LANES), jnp.int32),
                pltpu.VMEM((blocks, LANES), f32),
                pltpu.VMEM(((2 * CAP_X + 7) // 8 * 8, LANES), f32),
                pltpu.VMEM(((slots + 7) // 8 * 8, LANES), f32),
                pltpu.VMEM((2 * rows * halves, HALF), f32),
                pltpu.VMEM((2 * rows * halves * sends, HALF), f32),
                pltpu.VMEM((2, packed_x, LANES), f32),
                pltpu.VMEM((2, packed_x, LANES), f32),
                pltpu.VMEM((8, block_lists.shape[1]), f32),
                pltpu.VMEM((len(steps_z), 8, block_lists.shape[1]), f32),
                pltpu.VMEM((sends, sum_rows, HALF), f32),
                pltpu.VMEM((sends, sum_rows, HALF), f32),
                pltpu.SMEM(block_counts.shape, jnp.int32),
                pltpu.SMEM(block_lists.shape, jnp.int32),
                pltpu.VMEM(block_lists.shape, jnp.int32),
                pltpu.SemaphoreType.DMA((7,)),
                pltpu.SemaphoreType.DMA((2,)),
                pltpu.SemaphoreType.DMA((2,)),
                pltpu.SemaphoreType.DMA((len(steps_z),)),
                pltpu.SemaphoreType.DMA((len(steps_z),)),
                pltpu.SemaphoreType.DMA((sends,)),
                pltpu.SemaphoreType.DMA((sends,)),
            ],
            compiler_params=pltpu.CompilerParams(collective_id=0, has_side_effects=True),
        )(block_counts, block_lists, particle_fields, *by_block)

    placed = (
        P(None, AXES),
        P(AXES),
        P(AXES),
        P(AXES),
        P(AXES, None),
        P(AXES, None),
    )
    return jax.shard_map(
        per_device,
        mesh=mesh,
        in_specs=placed,
        out_specs=P(None, AXES),
        check_vma=False,
    )
```

```python
import functools

import jax
import jax.numpy as jnp
from jax import lax
from jax.experimental import pallas as pl
from jax.experimental.pallas import tpu as pltpu
from jax.sharding import PartitionSpec as P

CELLS = 512
CAP_X = 6
CAP_Z = 6
CAP_Y = 12
LANES = 128
HALF = 256
GROUP = 8
GONE = 16
AXES = ("gx", "gy", "gz")


def plan(sizes):
    steps_z = (1,) if sizes["gz"] == 2 else (-1, 1)
    classes = [{}, {"gy": -1}, {"gy": 1}]
    for dz in steps_z:
        classes += [{"gz": dz}, {"gz": dz, "gy": -1}, {"gz": dz, "gy": 1}]
    return steps_z, classes


def migrate_kernel(
    sizes,
    counts_hbm,
    lists_hbm,
    fields_hbm,
    step_hbm,
    live_hbm,
    cell_hbm,
    out_ref,
    fields,
    step,
    live,
    cell,
    offsets,
    offsets_x,
    offsets_slot,
    acc_kept,
    acc,
    alone,
    sent_x,
    got_x,
    sent_meta,
    got_meta,
    sent,
    got,
    counts,
    lists,
    lists_row,
    load_sem,
    send_x_sem,
    recv_x_sem,
    send_meta_sem,
    recv_meta_sem,
    send_sem,
    recv_sem,
    ready,
):
    steps_z, classes = plan(sizes)
    field_count = fields_hbm.shape[0]
    rows = (field_count + 1 + 7) // 8 * 8
    whole = field_count // 8 * 8
    tail = field_count - whole
    blocks = step.shape[0]
    halves = CELLS // HALF
    start_z, start_y = 2 * CAP_X, 2 * CAP_X + 2 * CAP_Z

    me = {axis: lax.axis_index(axis) for axis in AXES}

    def target(moves):
        return {a: lax.rem(me[a] + sizes[a] + d, sizes[a]) for a, d in moves.items()}

    def remote(src, dst, send, recv, moves):
        return pltpu.make_async_remote_copy(
            src_ref=src,
            dst_ref=dst,
            send_sem=send,
            recv_sem=recv,
            device_id=target(moves),
            device_id_type=pl.DeviceIdType.MESH,
        )

    loads = [
        pltpu.make_async_copy(src, dst, load_sem.at[i])
        for i, (src, dst) in enumerate(
            [
                (counts_hbm, counts),
                (lists_hbm, lists),
                (lists_hbm, lists_row),
                (step_hbm, step),
                (live_hbm, live),
                (cell_hbm, cell),
                (fields_hbm, fields),
            ]
        )
    ]
    for load in loads:
        load.start()

    moves_x = ({"gx": -1}, {"gx": 1})
    partners = {0: [], -1: [], 1: []}
    seen = set()
    for moves in list(moves_x) + classes[1:]:
        place = tuple(moves.get(a, 0) % sizes[a] for a in AXES)
        if place not in seen:
            seen.add(place)
            partners[moves.get("gy", 0) if sizes["gy"] > 2 else 0].append(moves)
    greets = {-1: me["gy"] == 0, 1: me["gy"] < sizes["gy"] - 1}
    barrier = pltpu.get_barrier_semaphore()

    def signal(semaphore, group):
        for moves in group:
            pl.semaphore_signal(
                semaphore, inc=1, device_id=target(moves), device_id_type=pl.DeviceIdType.MESH
            )

    signal(barrier, partners[0])
    for dy in (-1, 1):
        pl.when(greets[dy])(functools.partial(signal, barrier, partners[dy]))

    expected = len(partners[0])
    for dy in (-1, 1):
        expected += jnp.logical_not(greets[dy]).astype(jnp.int32) * len(partners[dy])

    for load in loads[:3]:
        load.wait()

    lane = lax.broadcasted_iota(jnp.int32, lists_row.shape, 1)
    z_number = blocks + 2 * CAP_X + jnp.where(
        lane < start_z + CAP_Z, lane - start_z + CAP_Z, lane - start_z - CAP_Z
    )
    onward = jnp.zeros(lists_row.shape, jnp.float32)
    for k in range(2 * CAP_Y):
        side, i = k // CAP_Y, k % CAP_Y
        count = jnp.full(lists_row.shape, counts[0, 4 + side])
        hit = (z_number == lists[0, start_y + k]) & (count > i)
        onward = jnp.where(hit, float(1 + side), onward)
    sent_meta[...] = jnp.broadcast_to(onward, sent_meta.shape)

    pl.semaphore_wait(barrier, expected)

    copies_meta = [
        remote(
            sent_meta, got_meta.at[i], send_meta_sem.at[i], recv_meta_sem.at[i], {"gz": dz}
        )
        for i, dz in enumerate(steps_z)
    ]
    for copy in copies_meta:
        copy.start()
    for dy in (-1, 1):
        heard = ready.at[(1 - dy) // 2]
        pl.when(jnp.logical_not(greets[dy]))(functools.partial(signal, heard, partners[dy]))

    for load in loads[3:]:
        load.wait()

    first_row = lax.broadcasted_iota(jnp.int32, (8, LANES), 0)

    def own_block(e):
        v = fields[:, pl.ds(e * LANES, LANES)]
        top = v[:8]
        pace = step[pl.ds(e, 1), :]
        top = top + jnp.where(first_row < 3, pace * pltpu.roll(top, 5, 0), 0.0)
        v = jnp.concatenate([top, v[8:]], axis=0)
        v = v * live[pl.ds(e, 1), :].astype(jnp.float32)
        where_to = cell[pl.ds(e, 1), :].astype(jnp.float32)
        return jnp.concatenate([v, v[whole:]], axis=0), where_to

    for slot in range(2 * CAP_X):
        block, where_to = own_block(jnp.minimum(lists[0, slot], blocks - 1))
        side, i = slot // CAP_X, slot % CAP_X
        count = jnp.full((rows, LANES), counts[0, side])
        block = jnp.where(count > i, block, 0.0)
        where_to = jnp.where(count[:1] > i, where_to, 0.0)
        sent_x[side, pl.ds(i * whole, whole), :] = block[:whole]
        sent_x[side, pl.ds(CAP_X * whole + i * tail, tail), :] = block[whole:field_count]
        sent_x[side, pl.ds(CAP_X * field_count + i, 1), :] = where_to

    def copy_x(side):
        return [
            remote(
                sent_x.at[pl.ds(s, 1)],
                got_x.at[pl.ds(s, 1)],
                send_x_sem.at[s],
                recv_x_sem.at[s],
                moves_x[s],
            )
            for s in side
        ]

    copies_x = copy_x((0, 1))
    for copy in copies_x:
        copy.start()

    spans = (CAP_X, CAP_X, CAP_Z, CAP_Z, CAP_Y, CAP_Y)
    limit = jnp.zeros(lists_row.shape, jnp.int32)
    away = jnp.zeros(lists_row.shape, jnp.float32)
    start = 0
    for k, span in enumerate(spans):
        here = lane >= start
        limit = jnp.where(here, counts[0, k] + start, limit)
        away = jnp.where(here, float(GONE if k < 4 else k - 3), away)
        start += span
    valid = lane < limit
    entries = lists_row[...]
    own_entry = valid & (entries < blocks)

    def table(ref, first, value, by_lane):
        number = first + lax.broadcasted_iota(jnp.int32, (ref.shape[0], lists_row.shape[1]), 0)
        hit = (lane if by_lane else entries) == number
        total = jnp.sum(jnp.where(hit, value, 0.0), axis=1, keepdims=True)
        ref[...] = jnp.broadcast_to(total, ref.shape)

    table(offsets, 0, jnp.where(valid, away, 0.0), False)
    y_slots = offsets_slot.at[pl.ds(2 * CAP_Z, 2 * CAP_Y)]
    table(y_slots, start_y, jnp.where(own_entry, away, float(GONE)), True)

    pack = 2 * 8
    bf16 = jnp.bfloat16
    row16 = lax.broadcasted_iota(jnp.int32, (pack, LANES), 0)
    code = row16.astype(jnp.float32)
    second = jnp.where(row16 >= 8, 1.0, 0.0)

    zero = jnp.zeros((pack, LANES), bf16)
    one = jnp.ones((pack, LANES), bf16)

    def prepared(v, cells):
        body, end = v[:whole], v[whole:]
        high = body.astype(bf16)
        low = (body - high.astype(jnp.float32)).astype(bf16)
        end_high = end.astype(bf16).astype(jnp.float32)
        end = jnp.where(first_row < tail, end_high, end - end_high)
        end = jnp.concatenate([end, end], axis=0).astype(bf16)
        part = jnp.floor(cells * (1.0 / HALF))
        ahead = (jnp.broadcast_to(cells - part * HALF, (pack, LANES)) - code).astype(bf16)
        right = [
            jnp.where(ahead == jnp.full((pack, LANES), k, bf16), one, zero)
            for k in range(0, HALF, pack)
        ]
        return high, low, end, part, jnp.concatenate(right, axis=0)

    def masked(block, kind, group):
        high, low, end, part, right = block
        part = jnp.broadcast_to(part + kind * halves, (pack, LANES))
        part_end = (part - second).astype(bf16)
        part = part.astype(bf16)
        left = []
        for c in group:
            for h in range(halves):
                here = part == jnp.full((pack, LANES), c * halves + h, bf16)
                left += [jnp.where(here, high, zero), jnp.where(here, low, zero)]
            here = part_end == jnp.full((pack, LANES), c * halves, bf16)
            left.append(jnp.where(here, end, zero))
        return jnp.concatenate(left, axis=0), right

    each = 2 * whole * halves + pack

    def span_of(group):
        return pl.ds((group[0] - 1) * each, len(group) * each)

    def product(pairs):
        left = jnp.concatenate([a for a, _ in pairs], axis=1)
        right = jnp.concatenate([b for _, b in pairs], axis=1)
        return lax.dot_general(
            left, right, (((1,), (1,)), ((), ())), preferred_element_type=jnp.float32
        )

    top_rows = lax.broadcasted_iota(jnp.int32, (8, HALF), 0) < tail

    def packed(r):
        out = []
        for h in range(halves):
            high = 2 * h * whole
            out.append(r[high : high + whole] + r[high + whole : high + 2 * whole])
        ends = [r[2 * halves * whole + 8 * h :][:8] for h in range(halves)]
        ends = [e + pltpu.roll(e, tail, 0) for e in ends]
        return out + [jnp.where(top_rows, ends[0], ends[1])]

    def own_slot(k):
        return prepared(*own_block(jnp.minimum(lists[0, start_z + k], blocks - 1)))

    def slot_kind(k):
        return offsets_slot[pl.ds(k, 1), :]

    for side in range(2):
        first = 2 * CAP_Z + side * CAP_Y
        slots = range(first, first + CAP_Y)
        pairs = [masked(own_slot(k), slot_kind(k), (1 + side,)) for k in slots]
        acc[span_of((1 + side,)), :] = product(pairs)

    def unpacked(side, i):
        body = got_x[side, pl.ds(i * whole, whole), :]
        rest = got_x[side, pl.ds(CAP_X * whole + i * tail, tail), :]
        cells = got_x[side, pl.ds(CAP_X * field_count + i, 1), :]
        return jnp.concatenate([body, rest, rest], axis=0), cells

    def wait_x(side):
        pltpu.make_async_remote_copy(
            src_ref=sent_x.at[pl.ds(side, 1)],
            dst_ref=got_x.at[pl.ds(side, 1)],
            send_sem=send_x_sem.at[side],
            recv_sem=recv_x_sem.at[side],
            device_id=target(moves_x[0]),
            device_id_type=pl.DeviceIdType.MESH,
        ).wait_recv()

    bound = tuple(range(1, len(classes)))
    y_classes, z_classes = bound[:2], bound[2:]
    near = lax.rem(me["gx"], 2)
    far = 1 - near

    def got_kind(ref, side, i):
        base = (1 - side) * CAP_X
        return ref[pl.ds(base + i, 1), :]

    def block_sums(ref, i, block):
        plain = masked(block, jnp.zeros((1, LANES), jnp.float32), (0,))
        ref[i] = jnp.concatenate(packed(product([plain])), axis=0)

    for k in range(2 * CAP_Z):
        block_sums(alone, k, own_slot(k))
    wait_x(near)
    near_blocks = [prepared(*unpacked(near, i)) for i in range(CAP_X)]
    for i, block in enumerate(near_blocks):
        block_sums(alone, 2 * CAP_Z + i, block)
    kinds = [got_kind(offsets.at[pl.ds(blocks, 2 * CAP_X)], near, i) for i in range(CAP_X)]
    pairs = [masked(v, kind, y_classes) for v, kind in zip(near_blocks, kinds)]
    acc[...] += product(pairs)

    for copy in copies_meta:
        copy.wait_recv()
    if len(steps_z) == 1:
        kind = got_meta[0, :1, :]
    else:
        kind = jnp.where(lane < start_z + CAP_Z, got_meta[1, :1, :], got_meta[0, :1, :] + 3.0)
    in_z = (lane >= start_z) & (lane < start_y)
    away = jnp.where(in_z, kind + 3.0, away)
    table(offsets_x, blocks, jnp.where(valid, away, 0.0), False)
    z_slots = offsets_slot.at[pl.ds(0, 2 * CAP_Z)]
    table(z_slots, start_z, jnp.where(own_entry, away, float(GONE)), True)

    kinds = [slot_kind(k) for k in range(2 * CAP_Z)]
    kinds += [got_kind(offsets_x, near, i) for i in range(CAP_X)]
    kinds = [jnp.concatenate([kind] * (HALF // LANES), axis=1) for kind in kinds]
    for c in z_classes:
        sent[c - 1] = sum(
            jnp.where(kind == float(c), alone[k], 0.0) for k, kind in enumerate(kinds)
        )

    wait_x(far)
    pairs = []
    for i in range(CAP_X):
        pairs.append(masked(prepared(*unpacked(far, i)), got_kind(offsets_x, far, i), bound))
    sums = product(pairs)
    for c in bound:
        total = sums[(c - 1) * each : c * each]
        if c in y_classes:
            total = total + acc[span_of((c,)), :]
        total = jnp.concatenate(packed(total), axis=0)
        sent[c - 1] = total + sent[c - 1] if c in z_classes else total

    def message(c, moves):
        return remote(sent.at[c], got.at[c], send_sem.at[c], recv_sem.at[c], moves)

    for dy in (-1, 1):
        heard = functools.partial(pl.semaphore_wait, ready.at[(1 + dy) // 2], len(partners[dy]))
        if partners[dy]:
            pl.when(greets[dy])(heard)
    side = jnp.where(me["gy"] == 0, 0, 1)
    copies = []
    for s in (side, 1 - side):
        for q, dz in enumerate(steps_z):
            copies.append(message(3 * q + 3 + s, {"gz": dz, "gy": 2 * s - 1}))
        copies.append(message(s, {"gy": 2 * s - 1}))
    for q, dz in enumerate(steps_z):
        copies.append(message(3 * q + 2, {"gz": dz}))
    for copy in copies:
        copy.start()

    acc_kept[...] = jnp.zeros_like(acc_kept)
    for side in range(2):
        pairs = []
        for i in range(CAP_X):
            pairs.append(masked(prepared(*unpacked(side, i)), got_kind(offsets_x, side, i), (0,)))
        acc_kept[...] += product(pairs)

    def bin_own(g, carry):
        pairs = []
        for i in range(GROUP):
            b = g * GROUP + i
            pairs.append(masked(prepared(*own_block(b)), offsets[pl.ds(b, 1), :], (0,)))
        acc_kept[...] += product(pairs)
        return carry

    lax.fori_loop(0, blocks // GROUP, bin_own, 0)

    total = jnp.concatenate(packed(acc_kept[...]), axis=0)
    for c in (3, 6, 1, 2, 4, 5, 7, 8):
        if c in bound:
            message(c - 1, classes[c]).wait_recv()
            total = total + got[c - 1]
    for h in range(halves):
        here = pl.ds(h * HALF, HALF)
        out_ref[:whole, here] = total[h * whole : (h + 1) * whole]
        last = halves * whole + h * tail
        out_ref[whole:, here] = total[last : last + tail]
    for copy in copies_x + copies_meta + copies:
        copy.wait_send()


def solution(mesh):
    sizes = {axis: mesh.shape[axis] for axis in AXES}

    def per_device(particle_fields, step_length, live_mask, dest_cell, block_counts, block_lists):
        field_count, particles = particle_fields.shape
        blocks = particles // LANES
        rows = (field_count + 1 + 7) // 8 * 8
        steps_z, classes = plan(sizes)
        sends = len(classes) - 1
        halves = CELLS // HALF
        sum_rows = (field_count * halves + 7) // 8 * 8
        packed_x = (CAP_X * (field_count + 1) + 7) // 8 * 8
        slots = 2 * CAP_Z + 2 * CAP_Y
        each = 2 * (field_count // 8 * 8) * halves + 16

        by_block = [a.reshape(blocks, LANES) for a in (step_length, live_mask, dest_cell)]
        any_space = pl.BlockSpec(memory_space=pl.ANY)
        f32 = jnp.float32
        return pl.pallas_call(
            functools.partial(migrate_kernel, sizes),
            out_shape=pltpu.VMEM((field_count, CELLS), f32),
            in_specs=[any_space] * 6,
            out_specs=pl.BlockSpec(memory_space=pltpu.VMEM),
            scratch_shapes=[
                pltpu.VMEM((field_count, particles), f32),
                pltpu.VMEM((blocks, LANES), f32),
                pltpu.VMEM((blocks, LANES), jnp.int32),
                pltpu.VMEM((blocks, LANES), jnp.int32),
                pltpu.VMEM((blocks + (2 * CAP_X + 7) // 8 * 8, LANES), f32),
                pltpu.VMEM(((2 * CAP_X + 7) // 8 * 8, LANES), f32),
                pltpu.VMEM(((slots + 7) // 8 * 8, LANES), f32),
                pltpu.VMEM((each, HALF), f32),
                pltpu.VMEM((each * 2, HALF), f32),
                pltpu.VMEM((2 * CAP_Z + CAP_X, sum_rows, HALF), f32),
                pltpu.VMEM((2, packed_x, LANES), f32),
                pltpu.VMEM((2, packed_x, LANES), f32),
                pltpu.VMEM((8, block_lists.shape[1]), f32),
                pltpu.VMEM((len(steps_z), 8, block_lists.shape[1]), f32),
                pltpu.VMEM((sends, sum_rows, HALF), f32),
                pltpu.VMEM((sends, sum_rows, HALF), f32),
                pltpu.SMEM(block_counts.shape, jnp.int32),
                pltpu.SMEM(block_lists.shape, jnp.int32),
                pltpu.VMEM(block_lists.shape, jnp.int32),
                pltpu.SemaphoreType.DMA((7,)),
                pltpu.SemaphoreType.DMA((2,)),
                pltpu.SemaphoreType.DMA((2,)),
                pltpu.SemaphoreType.DMA((len(steps_z),)),
                pltpu.SemaphoreType.DMA((len(steps_z),)),
                pltpu.SemaphoreType.DMA((sends,)),
                pltpu.SemaphoreType.DMA((sends,)),
                pltpu.SemaphoreType.REGULAR((2,)),
            ],
            compiler_params=pltpu.CompilerParams(collective_id=0, has_side_effects=True),
        )(block_counts, block_lists, particle_fields, *by_block)

    placed = (
        P(None, AXES),
        P(AXES),
        P(AXES),
        P(AXES),
        P(AXES, None),
        P(AXES, None),
    )
    return jax.shard_map(
        per_device,
        mesh=mesh,
        in_specs=placed,
        out_specs=P(None, AXES),
        check_vma=False,
    )
```

```python
import functools

import jax
import jax.numpy as jnp
from jax import lax
from jax.experimental import pallas as pl
from jax.experimental.pallas import tpu as pltpu
from jax.sharding import PartitionSpec as P

CELLS = 512
CAP_X = 6
CAP_Z = 6
CAP_Y = 12
LANES = 128
HALF = 256
GROUP = 8
GONE = 16
AXES = ("gx", "gy", "gz")


def plan(sizes):
    steps_z = (1,) if sizes["gz"] == 2 else (-1, 1)
    classes = [{}, {"gy": -1}, {"gy": 1}]
    for dz in steps_z:
        classes += [{"gz": dz}, {"gz": dz, "gy": -1}, {"gz": dz, "gy": 1}]
    return steps_z, classes


def migrate_kernel(
    sizes,
    counts_hbm,
    lists_hbm,
    fields_hbm,
    step_hbm,
    live_hbm,
    cell_hbm,
    out_ref,
    fields,
    step,
    live,
    cell,
    offsets,
    offsets_x,
    offsets_slot,
    acc_kept,
    acc,
    alone,
    sent_x,
    got_x,
    sent_meta,
    got_meta,
    sent,
    got,
    counts,
    lists,
    lists_row,
    load_sem,
    send_x_sem,
    recv_x_sem,
    send_meta_sem,
    recv_meta_sem,
    send_sem,
    recv_sem,
    ready,
):
    steps_z, classes = plan(sizes)
    field_count = fields_hbm.shape[0]
    rows = (field_count + 1 + 7) // 8 * 8
    whole = field_count // 8 * 8
    tail = field_count - whole
    blocks = step.shape[0]
    halves = CELLS // HALF
    start_z, start_y = 2 * CAP_X, 2 * CAP_X + 2 * CAP_Z

    me = {axis: lax.axis_index(axis) for axis in AXES}

    def target(moves):
        return {a: lax.rem(me[a] + sizes[a] + d, sizes[a]) for a, d in moves.items()}

    def remote(src, dst, send, recv, moves):
        return pltpu.make_async_remote_copy(
            src_ref=src,
            dst_ref=dst,
            send_sem=send,
            recv_sem=recv,
            device_id=target(moves),
            device_id_type=pl.DeviceIdType.MESH,
        )

    loads = [
        pltpu.make_async_copy(src, dst, load_sem.at[i])
        for i, (src, dst) in enumerate(
            [
                (counts_hbm, counts),
                (lists_hbm, lists),
                (lists_hbm, lists_row),
                (step_hbm, step),
                (live_hbm, live),
                (cell_hbm, cell),
                (fields_hbm, fields),
            ]
        )
    ]
    for load in loads:
        load.start()

    moves_x = ({"gx": -1}, {"gx": 1})
    partners = {0: [], -1: [], 1: []}
    seen = set()
    for moves in list(moves_x) + classes[1:]:
        place = tuple(moves.get(a, 0) % sizes[a] for a in AXES)
        if place not in seen:
            seen.add(place)
            partners[moves.get("gy", 0) if sizes["gy"] > 2 else 0].append(moves)
    greets = {-1: me["gy"] == 0, 1: me["gy"] < sizes["gy"] - 1}
    barrier = pltpu.get_barrier_semaphore()

    def signal(semaphore, group):
        for moves in group:
            pl.semaphore_signal(
                semaphore, inc=1, device_id=target(moves), device_id_type=pl.DeviceIdType.MESH
            )

    signal(barrier, partners[0])
    for dy in (-1, 1):
        pl.when(greets[dy])(functools.partial(signal, barrier, partners[dy]))

    expected = len(partners[0])
    for dy in (-1, 1):
        expected += jnp.logical_not(greets[dy]).astype(jnp.int32) * len(partners[dy])

    for load in loads[:3]:
        load.wait()

    lane = lax.broadcasted_iota(jnp.int32, lists_row.shape, 1)
    z_number = blocks + 2 * CAP_X + jnp.where(
        lane < start_z + CAP_Z, lane - start_z + CAP_Z, lane - start_z - CAP_Z
    )
    onward = jnp.zeros(lists_row.shape, jnp.float32)
    for k in range(2 * CAP_Y):
        side, i = k // CAP_Y, k % CAP_Y
        count = jnp.full(lists_row.shape, counts[0, 4 + side])
        hit = (z_number == lists[0, start_y + k]) & (count > i)
        onward = jnp.where(hit, float(1 + side), onward)
    sent_meta[...] = jnp.broadcast_to(onward, sent_meta.shape)

    pl.semaphore_wait(barrier, expected)

    copies_meta = [
        remote(
            sent_meta, got_meta.at[i], send_meta_sem.at[i], recv_meta_sem.at[i], {"gz": dz}
        )
        for i, dz in enumerate(steps_z)
    ]
    for copy in copies_meta:
        copy.start()
    for dy in (-1, 1):
        heard = ready.at[(1 - dy) // 2]
        pl.when(jnp.logical_not(greets[dy]))(functools.partial(signal, heard, partners[dy]))

    for load in loads[3:]:
        load.wait()

    first_row = lax.broadcasted_iota(jnp.int32, (8, LANES), 0)

    def own_block(e):
        v = fields[:, pl.ds(e * LANES, LANES)]
        top = v[:8]
        pace = step[pl.ds(e, 1), :]
        top = top + jnp.where(first_row < 3, pace * pltpu.roll(top, 5, 0), 0.0)
        v = jnp.concatenate([top, v[8:]], axis=0)
        v = v * live[pl.ds(e, 1), :].astype(jnp.float32)
        where_to = cell[pl.ds(e, 1), :].astype(jnp.float32)
        return jnp.concatenate([v, v[whole:]], axis=0), where_to

    for slot in range(2 * CAP_X):
        block, where_to = own_block(jnp.minimum(lists[0, slot], blocks - 1))
        side, i = slot // CAP_X, slot % CAP_X
        count = jnp.full((rows, LANES), counts[0, side])
        block = jnp.where(count > i, block, 0.0)
        where_to = jnp.where(count[:1] > i, where_to, 0.0)
        sent_x[side, pl.ds(i * whole, whole), :] = block[:whole]
        sent_x[side, pl.ds(CAP_X * whole + i * tail, tail), :] = block[whole:field_count]
        sent_x[side, pl.ds(CAP_X * field_count + i, 1), :] = where_to

    def copy_x(side):
        return [
            remote(
                sent_x.at[pl.ds(s, 1)],
                got_x.at[pl.ds(s, 1)],
                send_x_sem.at[s],
                recv_x_sem.at[s],
                moves_x[s],
            )
            for s in side
        ]

    copies_x = copy_x((0, 1))
    for copy in copies_x:
        copy.start()

    spans = (CAP_X, CAP_X, CAP_Z, CAP_Z, CAP_Y, CAP_Y)
    limit = jnp.zeros(lists_row.shape, jnp.int32)
    away = jnp.zeros(lists_row.shape, jnp.float32)
    start = 0
    for k, span in enumerate(spans):
        here = lane >= start
        limit = jnp.where(here, counts[0, k] + start, limit)
        away = jnp.where(here, float(GONE if k < 4 else k - 3), away)
        start += span
    valid = lane < limit
    entries = lists_row[...]
    own_entry = valid & (entries < blocks)

    def table(ref, first, value, by_lane):
        number = first + lax.broadcasted_iota(jnp.int32, (ref.shape[0], lists_row.shape[1]), 0)
        hit = (lane if by_lane else entries) == number
        total = jnp.sum(jnp.where(hit, value, 0.0), axis=1, keepdims=True)
        ref[...] = jnp.broadcast_to(total, ref.shape)

    table(offsets, 0, jnp.where(valid, away, 0.0), False)
    y_slots = offsets_slot.at[pl.ds(2 * CAP_Z, 2 * CAP_Y)]
    table(y_slots, start_y, jnp.where(own_entry, away, float(GONE)), True)

    pack = 2 * 8
    bf16 = jnp.bfloat16
    row16 = lax.broadcasted_iota(jnp.int32, (pack, LANES), 0)
    code = row16.astype(jnp.float32)
    second = jnp.where(row16 >= 8, 1.0, 0.0)

    zero = jnp.zeros((pack, LANES), bf16)
    one = jnp.ones((pack, LANES), bf16)

    def prepared(v, cells):
        body, end = v[:whole], v[whole:]
        high = body.astype(bf16)
        low = (body - high.astype(jnp.float32)).astype(bf16)
        end_high = end.astype(bf16).astype(jnp.float32)
        end = jnp.where(first_row < tail, end_high, end - end_high)
        end = jnp.concatenate([end, end], axis=0).astype(bf16)
        part = jnp.floor(cells * (1.0 / HALF))
        ahead = (jnp.broadcast_to(cells - part * HALF, (pack, LANES)) - code).astype(bf16)
        right = [
            jnp.where(ahead == jnp.full((pack, LANES), k, bf16), one, zero)
            for k in range(0, HALF, pack)
        ]
        return high, low, end, part, jnp.concatenate(right, axis=0)

    def masked(block, kind, group):
        high, low, end, part, right = block
        part = jnp.broadcast_to(part + kind * halves, (pack, LANES))
        part_end = (part - second).astype(bf16)
        part = part.astype(bf16)
        left = []
        for c in group:
            for h in range(halves):
                here = part == jnp.full((pack, LANES), c * halves + h, bf16)
                left += [jnp.where(here, high, zero), jnp.where(here, low, zero)]
            here = part_end == jnp.full((pack, LANES), c * halves, bf16)
            left.append(jnp.where(here, end, zero))
        return jnp.concatenate(left, axis=0), right

    each = 2 * whole * halves + pack

    def span_of(group):
        return pl.ds((group[0] - 1) * each, len(group) * each)

    def product(pairs):
        left = jnp.concatenate([a for a, _ in pairs], axis=1)
        right = jnp.concatenate([b for _, b in pairs], axis=1)
        return lax.dot_general(
            left, right, (((1,), (1,)), ((), ())), preferred_element_type=jnp.float32
        )

    top_rows = lax.broadcasted_iota(jnp.int32, (8, HALF), 0) < tail

    def packed(r):
        out = []
        for h in range(halves):
            high = 2 * h * whole
            out.append(r[high : high + whole] + r[high + whole : high + 2 * whole])
        ends = [r[2 * halves * whole + 8 * h :][:8] for h in range(halves)]
        ends = [e + pltpu.roll(e, tail, 0) for e in ends]
        return out + [jnp.where(top_rows, ends[0], ends[1])]

    def spread(blocks, kinds, group):
        half = len(blocks) // 2
        minus = [(-high, -low, -end, *rest) for high, low, end, *rest in blocks[half:]]
        pairs = [masked(v, kind, group) for v, kind in zip(blocks[:half] + minus, kinds)]
        return product(pairs[:half]) - product(pairs[half:])

    def own_slot(k):
        return prepared(*own_block(jnp.minimum(lists[0, start_z + k], blocks - 1)))

    def slot_kind(k):
        return offsets_slot[pl.ds(k, 1), :]

    for side in range(2):
        first = 2 * CAP_Z + side * CAP_Y
        slots = range(first, first + CAP_Y)
        pairs = [masked(own_slot(k), slot_kind(k), (1 + side,)) for k in slots]
        acc[span_of((1 + side,)), :] = product(pairs)

    def unpacked(side, i):
        body = got_x[side, pl.ds(i * whole, whole), :]
        rest = got_x[side, pl.ds(CAP_X * whole + i * tail, tail), :]
        cells = got_x[side, pl.ds(CAP_X * field_count + i, 1), :]
        return jnp.concatenate([body, rest, rest], axis=0), cells

    def wait_x(side):
        pltpu.make_async_remote_copy(
            src_ref=sent_x.at[pl.ds(side, 1)],
            dst_ref=got_x.at[pl.ds(side, 1)],
            send_sem=send_x_sem.at[side],
            recv_sem=recv_x_sem.at[side],
            device_id=target(moves_x[0]),
            device_id_type=pl.DeviceIdType.MESH,
        ).wait_recv()

    bound = tuple(range(1, len(classes)))
    y_classes, z_classes = bound[:2], bound[2:]
    near = lax.rem(me["gx"], 2)
    far = 1 - near

    def got_kind(ref, side, i):
        base = (1 - side) * CAP_X
        return ref[pl.ds(base + i, 1), :]

    def block_sums(ref, i, block):
        plain = masked(block, jnp.zeros((1, LANES), jnp.float32), (0,))
        ref[i] = jnp.concatenate(packed(product([plain])), axis=0)

    for k in range(2 * CAP_Z):
        block_sums(alone, k, own_slot(k))
    wait_x(near)
    near_blocks = [prepared(*unpacked(near, i)) for i in range(CAP_X)]
    for i, block in enumerate(near_blocks):
        block_sums(alone, 2 * CAP_Z + i, block)
    kinds = [got_kind(offsets.at[pl.ds(blocks, 2 * CAP_X)], near, i) for i in range(CAP_X)]
    acc[...] += spread(near_blocks, kinds, y_classes)

    for copy in copies_meta:
        copy.wait_recv()
    if len(steps_z) == 1:
        kind = got_meta[0, :1, :]
    else:
        kind = jnp.where(lane < start_z + CAP_Z, got_meta[1, :1, :], got_meta[0, :1, :] + 3.0)
    in_z = (lane >= start_z) & (lane < start_y)
    away = jnp.where(in_z, kind + 3.0, away)
    table(offsets_x, blocks, jnp.where(valid, away, 0.0), False)
    z_slots = offsets_slot.at[pl.ds(0, 2 * CAP_Z)]
    table(z_slots, start_z, jnp.where(own_entry, away, float(GONE)), True)

    kinds = [slot_kind(k) for k in range(2 * CAP_Z)]
    kinds += [got_kind(offsets_x, near, i) for i in range(CAP_X)]
    kinds = [jnp.concatenate([kind] * (HALF // LANES), axis=1) for kind in kinds]
    for c in z_classes:
        sent[c - 1] = sum(
            jnp.where(kind == float(c), alone[k], 0.0) for k, kind in enumerate(kinds)
        )

    acc_kept[...] = jnp.zeros_like(acc_kept)

    def bin_own(g, carry):
        numbers = [g * GROUP + i for i in range(GROUP)]
        kinds = [offsets[pl.ds(b, 1), :] for b in numbers]
        acc_kept[...] += spread([prepared(*own_block(b)) for b in numbers], kinds, (0,))
        return carry

    wait_x(far)
    far_blocks = [prepared(*unpacked(far, i)) for i in range(CAP_X)]

    def finish(group):
        sums = spread(far_blocks, [got_kind(offsets_x, far, i) for i in range(CAP_X)], group)
        for g, c in enumerate(group):
            total = sums[g * each : (g + 1) * each]
            if c in y_classes:
                total = total + acc[span_of((c,)), :]
            total = jnp.concatenate(packed(total), axis=0)
            sent[c - 1] = total + sent[c - 1] if c in z_classes else total

    def message(c, moves):
        return remote(sent.at[c], got.at[c], send_sem.at[c], recv_sem.at[c], moves)

    side = jnp.where(me["gy"] == sizes["gy"] - 1, 1, 0)
    across = [c for c in bound if len(classes[c]) == 2]
    finish(across)
    for dy in (-1, 1):
        heard = functools.partial(pl.semaphore_wait, ready.at[(1 + dy) // 2], len(partners[dy]))
        if partners[dy]:
            pl.when(greets[dy])(heard)
    first = [
        message(3 * q + 3 + side, {"gz": dz, "gy": 2 * side - 1}) for q, dz in enumerate(steps_z)
    ]
    held = jnp.where(near == 1, 1, 0)
    lax.fori_loop(0, held, bin_own, 0)
    for copy in first:
        copy.start()
    finish([c for c in bound if c not in across])
    rest = [message(side, {"gy": 2 * side - 1})]
    for q, dz in enumerate(steps_z):
        rest.append(message(3 * q + 4 - side, {"gz": dz, "gy": 1 - 2 * side}))
    rest.append(message(1 - side, {"gy": 1 - 2 * side}))
    for q, dz in enumerate(steps_z):
        rest.append(message(3 * q + 2, {"gz": dz}))
    for copy in rest:
        copy.start()
    copies = first + rest

    for side in range(2):
        pairs = []
        for i in range(CAP_X):
            pairs.append(masked(prepared(*unpacked(side, i)), got_kind(offsets_x, side, i), (0,)))
        acc_kept[...] += product(pairs)

    lax.fori_loop(held, blocks // GROUP, bin_own, 0)

    total = jnp.concatenate(packed(acc_kept[...]), axis=0)
    for copy in copies_x + copies_meta + copies:
        copy.wait_send()
    for c in (3, 6, 1, 2, 4, 5, 7, 8):
        if c in bound:
            message(c - 1, classes[c]).wait_recv()
            total = total + got[c - 1]
    for h in range(halves):
        here = pl.ds(h * HALF, HALF)
        out_ref[:whole, here] = total[h * whole : (h + 1) * whole]
        last = halves * whole + h * tail
        out_ref[whole:, here] = total[last : last + tail]


def solution(mesh):
    sizes = {axis: mesh.shape[axis] for axis in AXES}

    def per_device(particle_fields, step_length, live_mask, dest_cell, block_counts, block_lists):
        field_count, particles = particle_fields.shape
        blocks = particles // LANES
        rows = (field_count + 1 + 7) // 8 * 8
        steps_z, classes = plan(sizes)
        sends = len(classes) - 1
        halves = CELLS // HALF
        sum_rows = (field_count * halves + 7) // 8 * 8
        packed_x = (CAP_X * (field_count + 1) + 7) // 8 * 8
        slots = 2 * CAP_Z + 2 * CAP_Y
        each = 2 * (field_count // 8 * 8) * halves + 16

        by_block = [a.reshape(blocks, LANES) for a in (step_length, live_mask, dest_cell)]
        any_space = pl.BlockSpec(memory_space=pl.ANY)
        f32 = jnp.float32
        return pl.pallas_call(
            functools.partial(migrate_kernel, sizes),
            out_shape=pltpu.VMEM((field_count, CELLS), f32),
            in_specs=[any_space] * 6,
            out_specs=pl.BlockSpec(memory_space=pltpu.VMEM),
            scratch_shapes=[
                pltpu.VMEM((field_count, particles), f32),
                pltpu.VMEM((blocks, LANES), f32),
                pltpu.VMEM((blocks, LANES), jnp.int32),
                pltpu.VMEM((blocks, LANES), jnp.int32),
                pltpu.VMEM((blocks + (2 * CAP_X + 7) // 8 * 8, LANES), f32),
                pltpu.VMEM(((2 * CAP_X + 7) // 8 * 8, LANES), f32),
                pltpu.VMEM(((slots + 7) // 8 * 8, LANES), f32),
                pltpu.VMEM((each, HALF), f32),
                pltpu.VMEM((each * 2, HALF), f32),
                pltpu.VMEM((2 * CAP_Z + CAP_X, sum_rows, HALF), f32),
                pltpu.VMEM((2, packed_x, LANES), f32),
                pltpu.VMEM((2, packed_x, LANES), f32),
                pltpu.VMEM((8, block_lists.shape[1]), f32),
                pltpu.VMEM((len(steps_z), 8, block_lists.shape[1]), f32),
                pltpu.VMEM((sends, sum_rows, HALF), f32),
                pltpu.VMEM((sends, sum_rows, HALF), f32),
                pltpu.SMEM(block_counts.shape, jnp.int32),
                pltpu.SMEM(block_lists.shape, jnp.int32),
                pltpu.VMEM(block_lists.shape, jnp.int32),
                pltpu.SemaphoreType.DMA((7,)),
                pltpu.SemaphoreType.DMA((2,)),
                pltpu.SemaphoreType.DMA((2,)),
                pltpu.SemaphoreType.DMA((len(steps_z),)),
                pltpu.SemaphoreType.DMA((len(steps_z),)),
                pltpu.SemaphoreType.DMA((sends,)),
                pltpu.SemaphoreType.DMA((sends,)),
                pltpu.SemaphoreType.REGULAR((2,)),
            ],
            compiler_params=pltpu.CompilerParams(collective_id=0, has_side_effects=True),
        )(block_counts, block_lists, particle_fields, *by_block)

    placed = (
        P(None, AXES),
        P(AXES),
        P(AXES),
        P(AXES),
        P(AXES, None),
        P(AXES, None),
    )
    return jax.shard_map(
        per_device,
        mesh=mesh,
        in_specs=placed,
        out_specs=P(None, AXES),
        check_vma=False,
    )
```

```python
import functools

import jax
import jax.numpy as jnp
from jax import lax
from jax.experimental import pallas as pl
from jax.experimental.pallas import tpu as pltpu
from jax.sharding import PartitionSpec as P

CELLS = 512
CAP_X = 6
CAP_Z = 6
CAP_Y = 12
LANES = 128
HALF = 256
GROUP = 8
GONE = 16
AXES = ("gx", "gy", "gz")


def plan(sizes):
    steps_z = (1,) if sizes["gz"] == 2 else (-1, 1)
    classes = [{}, {"gy": -1}, {"gy": 1}]
    for dz in steps_z:
        classes += [{"gz": dz}, {"gz": dz, "gy": -1}, {"gz": dz, "gy": 1}]
    return steps_z, classes


def migrate_kernel(
    sizes,
    counts_hbm,
    lists_hbm,
    fields_hbm,
    step_hbm,
    live_hbm,
    cell_hbm,
    out_ref,
    bodies,
    ends,
    step,
    live,
    cell,
    offsets,
    offsets_x,
    offsets_slot,
    acc_kept,
    acc,
    alone,
    sent_x,
    got_x,
    sent_meta,
    got_meta,
    sent,
    got,
    counts,
    lists,
    lists_row,
    load_sem,
    send_x_sem,
    recv_x_sem,
    send_meta_sem,
    recv_meta_sem,
    send_sem,
    recv_sem,
    ready,
):
    steps_z, classes = plan(sizes)
    field_count = fields_hbm.shape[0]
    rows = (field_count + 1 + 7) // 8 * 8
    whole = field_count // 8 * 8
    tail = field_count - whole
    blocks = step.shape[0]
    halves = CELLS // HALF
    start_z, start_y = 2 * CAP_X, 2 * CAP_X + 2 * CAP_Z

    me = {axis: lax.axis_index(axis) for axis in AXES}

    def target(moves):
        return {a: lax.rem(me[a] + sizes[a] + d, sizes[a]) for a, d in moves.items()}

    def remote(src, dst, send, recv, moves):
        return pltpu.make_async_remote_copy(
            src_ref=src,
            dst_ref=dst,
            send_sem=send,
            recv_sem=recv,
            device_id=target(moves),
            device_id_type=pl.DeviceIdType.MESH,
        )

    loads = [
        pltpu.make_async_copy(src, dst, load_sem.at[i])
        for i, (src, dst) in enumerate(
            [
                (counts_hbm, counts),
                (lists_hbm, lists),
                (lists_hbm, lists_row),
                (step_hbm, step),
                (live_hbm, live),
                (fields_hbm.at[pl.ds(0, whole)], bodies),
                (cell_hbm, cell),
                (fields_hbm.at[pl.ds(whole, tail)], ends),
            ]
        )
    ]
    for load in loads:
        load.start()

    moves_x = ({"gx": -1}, {"gx": 1})
    partners = {0: [], -1: [], 1: []}
    seen = set()
    for moves in list(moves_x) + classes[1:]:
        place = tuple(moves.get(a, 0) % sizes[a] for a in AXES)
        if place not in seen:
            seen.add(place)
            partners[moves.get("gy", 0) if sizes["gy"] > 2 else 0].append(moves)
    greets = {-1: me["gy"] == 0, 1: me["gy"] < sizes["gy"] - 1}
    barrier = pltpu.get_barrier_semaphore()

    def signal(semaphore, group):
        for moves in group:
            pl.semaphore_signal(
                semaphore, inc=1, device_id=target(moves), device_id_type=pl.DeviceIdType.MESH
            )

    signal(barrier, partners[0])
    for dy in (-1, 1):
        pl.when(greets[dy])(functools.partial(signal, barrier, partners[dy]))

    expected = len(partners[0])
    for dy in (-1, 1):
        expected += jnp.logical_not(greets[dy]).astype(jnp.int32) * len(partners[dy])

    for load in loads[:3]:
        load.wait()

    lane = lax.broadcasted_iota(jnp.int32, lists_row.shape, 1)
    z_number = blocks + 2 * CAP_X + jnp.where(
        lane < start_z + CAP_Z, lane - start_z + CAP_Z, lane - start_z - CAP_Z
    )
    onward = jnp.zeros(lists_row.shape, jnp.float32)
    for k in range(2 * CAP_Y):
        side, i = k // CAP_Y, k % CAP_Y
        count = jnp.full(lists_row.shape, counts[0, 4 + side])
        hit = (z_number == lists[0, start_y + k]) & (count > i)
        onward = jnp.where(hit, float(1 + side), onward)
    sent_meta[...] = jnp.broadcast_to(onward, sent_meta.shape)

    pl.semaphore_wait(barrier, expected)

    copies_meta = [
        remote(
            sent_meta, got_meta.at[i], send_meta_sem.at[i], recv_meta_sem.at[i], {"gz": dz}
        )
        for i, dz in enumerate(steps_z)
    ]
    for copy in copies_meta:
        copy.start()
    for dy in (-1, 1):
        heard = ready.at[(1 - dy) // 2]
        pl.when(jnp.logical_not(greets[dy]))(functools.partial(signal, heard, partners[dy]))

    first_row = lax.broadcasted_iota(jnp.int32, (8, LANES), 0)

    def columns(e):
        return pl.ds(e * LANES, LANES)

    def alive(e):
        return live[pl.ds(e, 1), :].astype(jnp.float32)

    def own_body(e):
        v = bodies[:, columns(e)]
        top = v[:8]
        top = top + jnp.where(first_row < 3, step[pl.ds(e, 1), :] * pltpu.roll(top, 5, 0), 0.0)
        return jnp.concatenate([top, v[8:]], axis=0) * alive(e)

    def own_end(e):
        return ends[:, columns(e)] * alive(e), cell[pl.ds(e, 1), :].astype(jnp.float32)

    def own_block(e):
        end, where_to = own_end(e)
        return jnp.concatenate([own_body(e), end, end], axis=0), where_to

    def leaving(slot):
        side, i = slot // CAP_X, slot % CAP_X
        return side, i, jnp.minimum(lists[0, slot], blocks - 1), counts[0, side]

    def copies_of(first, count):
        part = pl.ds(first, count)
        return [
            remote(
                sent_x.at[s, part], got_x.at[s, part], send_x_sem, recv_x_sem.at[s], moves_x[s]
            )
            for s in range(2)
        ]

    body_rows = CAP_X * whole
    copies_x = copies_of(0, body_rows) + copies_of(body_rows, sent_x.shape[1] - body_rows)
    for load in loads[3:6]:
        load.wait()
    for slot in range(2 * CAP_X):
        side, i, e, count = leaving(slot)
        block = jnp.where(jnp.full((whole, LANES), count) > i, own_body(e), 0.0)
        sent_x[side, pl.ds(i * whole, whole), :] = block
    for copy in copies_x[:2]:
        copy.start()
    for load in loads[6:]:
        load.wait()
    for slot in range(2 * CAP_X):
        side, i, e, count = leaving(slot)
        end, where_to = own_end(e)
        taken = jnp.full((tail, LANES), count) > i
        sent_x[side, pl.ds(body_rows + i * tail, tail), :] = jnp.where(taken, end, 0.0)
        where_to = jnp.where(taken[:1], where_to, 0.0)
        sent_x[side, pl.ds(CAP_X * field_count + i, 1), :] = where_to
    for copy in copies_x[2:]:
        copy.start()

    spans = (CAP_X, CAP_X, CAP_Z, CAP_Z, CAP_Y, CAP_Y)
    limit = jnp.zeros(lists_row.shape, jnp.int32)
    away = jnp.zeros(lists_row.shape, jnp.float32)
    start = 0
    for k, span in enumerate(spans):
        here = lane >= start
        limit = jnp.where(here, counts[0, k] + start, limit)
        away = jnp.where(here, float(GONE if k < 4 else k - 3), away)
        start += span
    valid = lane < limit
    entries = lists_row[...]
    own_entry = valid & (entries < blocks)

    def table(ref, first, value, by_lane):
        number = first + lax.broadcasted_iota(jnp.int32, (ref.shape[0], lists_row.shape[1]), 0)
        hit = (lane if by_lane else entries) == number
        total = jnp.sum(jnp.where(hit, value, 0.0), axis=1, keepdims=True)
        ref[...] = jnp.broadcast_to(total, ref.shape)

    table(offsets, 0, jnp.where(valid, away, 0.0), False)
    y_slots = offsets_slot.at[pl.ds(2 * CAP_Z, 2 * CAP_Y)]
    table(y_slots, start_y, jnp.where(own_entry, away, float(GONE)), True)

    pack = 2 * 8
    bf16 = jnp.bfloat16
    row16 = lax.broadcasted_iota(jnp.int32, (pack, LANES), 0)
    code = row16.astype(jnp.float32)
    second = jnp.where(row16 >= 8, 1.0, 0.0)

    zero = jnp.zeros((pack, LANES), bf16)
    one = jnp.ones((pack, LANES), bf16)

    def prepared(v, cells):
        body, end = v[:whole], v[whole:]
        high = body.astype(bf16)
        low = (body - high.astype(jnp.float32)).astype(bf16)
        end_high = end.astype(bf16).astype(jnp.float32)
        end = jnp.where(first_row < tail, end_high, end - end_high)
        end = jnp.concatenate([end, end], axis=0).astype(bf16)
        part = jnp.floor(cells * (1.0 / HALF))
        ahead = (jnp.broadcast_to(cells - part * HALF, (pack, LANES)) - code).astype(bf16)
        right = [
            jnp.where(ahead == jnp.full((pack, LANES), k, bf16), one, zero)
            for k in range(0, HALF, pack)
        ]
        return high, low, end, part, jnp.concatenate(right, axis=0)

    def level(number):
        return jnp.full((pack, LANES), number, jnp.float32).astype(bf16)

    def masked(block, kind, group):
        high, low, end, part, right = block
        part = jnp.broadcast_to(part + kind * halves, (pack, LANES))
        part_end = (part - second).astype(bf16)
        part = part.astype(bf16)
        left = []
        for c in group:
            for h in range(halves):
                here = part == level(c * halves + h)
                left += [jnp.where(here, high, zero), jnp.where(here, low, zero)]
            here = part_end == level(c * halves)
            left.append(jnp.where(here, end, zero))
        return jnp.concatenate(left, axis=0), right

    each = 2 * whole * halves + pack

    def span_of(group):
        return pl.ds((group[0] - 1) * each, len(group) * each)

    def product(pairs):
        left = jnp.concatenate([a for a, _ in pairs], axis=1)
        right = jnp.concatenate([b for _, b in pairs], axis=1)
        return lax.dot_general(
            left, right, (((1,), (1,)), ((), ())), preferred_element_type=jnp.float32
        )

    top_rows = lax.broadcasted_iota(jnp.int32, (8, HALF), 0) < tail

    def packed(r):
        out = []
        for h in range(halves):
            high = 2 * h * whole
            out.append(r[high : high + whole] + r[high + whole : high + 2 * whole])
        ends = [r[2 * halves * whole + 8 * h :][:8] for h in range(halves)]
        ends = [e + pltpu.roll(e, tail, 0) for e in ends]
        return out + [jnp.where(top_rows, ends[0], ends[1])]

    def spread(blocks, kinds, group):
        half = len(blocks) // 2
        minus = [(-high, -low, -end, *rest) for high, low, end, *rest in blocks[half:]]
        pairs = [masked(v, kind, group) for v, kind in zip(blocks[:half] + minus, kinds)]
        return product(pairs[:half]) - product(pairs[half:])

    def own_slot(k):
        return prepared(*own_block(jnp.minimum(lists[0, start_z + k], blocks - 1)))

    def slot_kind(k):
        return offsets_slot[pl.ds(k, 1), :]

    for side in range(2):
        first = 2 * CAP_Z + side * CAP_Y
        slots = range(first, first + CAP_Y)
        pairs = [masked(own_slot(k), slot_kind(k), (1 + side,)) for k in slots]
        acc[span_of((1 + side,)), :] = product(pairs)

    def unpacked(side, i):
        body = got_x[side, pl.ds(i * whole, whole), :]
        rest = got_x[side, pl.ds(CAP_X * whole + i * tail, tail), :]
        cells = got_x[side, pl.ds(CAP_X * field_count + i, 1), :]
        return jnp.concatenate([body, rest, rest], axis=0), cells

    def wait_x(side):
        pltpu.make_async_remote_copy(
            src_ref=sent_x.at[pl.ds(side, 1)],
            dst_ref=got_x.at[pl.ds(side, 1)],
            send_sem=send_x_sem,
            recv_sem=recv_x_sem.at[side],
            device_id=target(moves_x[0]),
            device_id_type=pl.DeviceIdType.MESH,
        ).wait_recv()

    bound = tuple(range(1, len(classes)))
    y_classes, z_classes = bound[:2], bound[2:]
    near = lax.rem(me["gx"], 2)
    far = 1 - near

    def got_kind(ref, side, i):
        base = (1 - side) * CAP_X
        return ref[pl.ds(base + i, 1), :]

    def block_sums(ref, i, block):
        plain = masked(block, jnp.zeros((1, LANES), jnp.float32), (0,))
        ref[i] = jnp.concatenate(packed(product([plain])), axis=0)

    for k in range(2 * CAP_Z):
        block_sums(alone, k, own_slot(k))
    wait_x(near)
    near_blocks = [prepared(*unpacked(near, i)) for i in range(CAP_X)]
    for i, block in enumerate(near_blocks):
        block_sums(alone, 2 * CAP_Z + i, block)
    kinds = [got_kind(offsets.at[pl.ds(blocks, 2 * CAP_X)], near, i) for i in range(CAP_X)]
    more = spread(near_blocks, kinds, y_classes)
    for c in y_classes:
        total = acc[span_of((c,)), :] + more[(c - 1) * each : c * each]
        sent[c - 1] = jnp.concatenate(packed(total), axis=0)

    for copy in copies_meta:
        copy.wait_recv()
    if len(steps_z) == 1:
        kind = got_meta[0, :1, :]
    else:
        kind = jnp.where(lane < start_z + CAP_Z, got_meta[1, :1, :], got_meta[0, :1, :] + 3.0)
    in_z = (lane >= start_z) & (lane < start_y)
    away = jnp.where(in_z, kind + 3.0, away)
    table(offsets_x, blocks, jnp.where(valid, away, 0.0), False)
    z_slots = offsets_slot.at[pl.ds(0, 2 * CAP_Z)]
    table(z_slots, start_z, jnp.where(own_entry, away, float(GONE)), True)

    kinds = [slot_kind(k) for k in range(2 * CAP_Z)]
    kinds += [got_kind(offsets_x, near, i) for i in range(CAP_X)]
    kinds = [jnp.concatenate([kind] * (HALF // LANES), axis=1) for kind in kinds]
    for c in z_classes:
        sent[c - 1] = sum(
            jnp.where(kind == float(c), alone[k], 0.0) for k, kind in enumerate(kinds)
        )

    acc_kept[...] = jnp.zeros_like(acc_kept)

    def bin_own(g, carry):
        numbers = [g * GROUP + i for i in range(GROUP)]
        kinds = [offsets[pl.ds(b, 1), :] for b in numbers]
        acc_kept[...] += spread([prepared(*own_block(b)) for b in numbers], kinds, (0,))
        return carry

    wait_x(far)
    far_blocks = [prepared(*unpacked(far, i)) for i in range(CAP_X)]

    def finish(group):
        sums = spread(far_blocks, [got_kind(offsets_x, far, i) for i in range(CAP_X)], group)
        for g, c in enumerate(group):
            pieces = packed(sums[g * each : (g + 1) * each])
            sent[c - 1] += jnp.concatenate(pieces, axis=0)

    def message(c, moves):
        return remote(sent.at[c - 1], got.at[c - 1], send_sem, recv_sem, moves)

    side = jnp.where(me["gy"] == sizes["gy"] - 1, 1, 0)
    along, across = (1, {}), [(3 * q + 4, {"gz": dz}) for q, dz in enumerate(steps_z)]
    straight = [(3 * q + 3, {"gz": dz}) for q, dz in enumerate(steps_z)]
    if len(steps_z) == 1:
        lead = jnp.where(me["gz"] == 0, 0, 1)
        ahead = [(1 + 3 * lead, {"gz": lead})]
        behind = [(4 - 3 * lead, {"gz": 1 - lead})]
    else:
        ahead, behind = across, [along]

    def on_side(group, s):
        return [message(c + s, moves | {"gy": 2 * s - 1}) for c, moves in group]

    finish([c + side for c, _ in ahead])
    for dy in (-1, 1):
        heard = functools.partial(pl.semaphore_wait, ready.at[(1 + dy) // 2], len(partners[dy]))
        if partners[dy]:
            pl.when(greets[dy])(heard)
    first = on_side(ahead, side)
    held = jnp.where(near == 1, 1, 0)
    lax.fori_loop(0, held, bin_own, 0)
    for copy in first:
        copy.start()
    finish([c + s for c, _ in behind for s in (0, 1)] + [c + 1 - side for c, _ in ahead] + [c for c, _ in straight])
    rest = on_side(behind, side)
    for copy in rest:
        copy.start()
    later = held + 2
    lax.fori_loop(held, later, bin_own, 0)
    direct = on_side(ahead, 1 - side) + on_side(behind, 1 - side)
    direct += [message(c, moves) for c, moves in straight]
    for copy in direct:
        copy.start()
    rest += direct
    copies = first + rest

    for side in range(2):
        pairs = []
        for i in range(CAP_X):
            pairs.append(masked(prepared(*unpacked(side, i)), got_kind(offsets_x, side, i), (0,)))
        acc_kept[...] += product(pairs)

    lax.fori_loop(later, blocks // GROUP, bin_own, 0)

    total = jnp.concatenate(packed(acc_kept[...]), axis=0)
    remote(sent_x, got_x, send_x_sem, recv_x_sem.at[0], moves_x[0]).wait_send()
    for copy in copies_meta:
        copy.wait_send()
    everything = remote(sent, got, send_sem, recv_sem, classes[1])
    everything.wait_send()
    everything.wait_recv()
    for c in bound:
        total = total + got[c - 1]
    for h in range(halves):
        here = pl.ds(h * HALF, HALF)
        out_ref[:whole, here] = total[h * whole : (h + 1) * whole]
        last = halves * whole + h * tail
        out_ref[whole:, here] = total[last : last + tail]


def solution(mesh):
    sizes = {axis: mesh.shape[axis] for axis in AXES}

    def per_device(particle_fields, step_length, live_mask, dest_cell, block_counts, block_lists):
        field_count, particles = particle_fields.shape
        blocks = particles // LANES
        rows = (field_count + 1 + 7) // 8 * 8
        steps_z, classes = plan(sizes)
        sends = len(classes) - 1
        halves = CELLS // HALF
        sum_rows = (field_count * halves + 7) // 8 * 8
        packed_x = (CAP_X * (field_count + 1) + 7) // 8 * 8
        slots = 2 * CAP_Z + 2 * CAP_Y
        each = 2 * (field_count // 8 * 8) * halves + 16

        by_block = [a.reshape(blocks, LANES) for a in (step_length, live_mask, dest_cell)]
        any_space = pl.BlockSpec(memory_space=pl.ANY)
        f32 = jnp.float32
        return pl.pallas_call(
            functools.partial(migrate_kernel, sizes),
            out_shape=pltpu.VMEM((field_count, CELLS), f32),
            in_specs=[any_space] * 6,
            out_specs=pl.BlockSpec(memory_space=pltpu.VMEM),
            scratch_shapes=[
                pltpu.VMEM((field_count // 8 * 8, particles), f32),
                pltpu.VMEM((field_count % 8, particles), f32),
                pltpu.VMEM((blocks, LANES), f32),
                pltpu.VMEM((blocks, LANES), jnp.int32),
                pltpu.VMEM((blocks, LANES), jnp.int32),
                pltpu.VMEM((blocks + (2 * CAP_X + 7) // 8 * 8, LANES), f32),
                pltpu.VMEM(((2 * CAP_X + 7) // 8 * 8, LANES), f32),
                pltpu.VMEM(((slots + 7) // 8 * 8, LANES), f32),
                pltpu.VMEM((each, HALF), f32),
                pltpu.VMEM((each * 2, HALF), f32),
                pltpu.VMEM((2 * CAP_Z + CAP_X, sum_rows, HALF), f32),
                pltpu.VMEM((2, packed_x, LANES), f32),
                pltpu.VMEM((2, packed_x, LANES), f32),
                pltpu.VMEM((8, block_lists.shape[1]), f32),
                pltpu.VMEM((len(steps_z), 8, block_lists.shape[1]), f32),
                pltpu.VMEM((sends, sum_rows, HALF), f32),
                pltpu.VMEM((sends, sum_rows, HALF), f32),
                pltpu.SMEM(block_counts.shape, jnp.int32),
                pltpu.SMEM(block_lists.shape, jnp.int32),
                pltpu.VMEM(block_lists.shape, jnp.int32),
                pltpu.SemaphoreType.DMA((8,)),
                pltpu.SemaphoreType.DMA,
                pltpu.SemaphoreType.DMA((2,)),
                pltpu.SemaphoreType.DMA((len(steps_z),)),
                pltpu.SemaphoreType.DMA((len(steps_z),)),
                pltpu.SemaphoreType.DMA,
                pltpu.SemaphoreType.DMA,
                pltpu.SemaphoreType.REGULAR((2,)),
            ],
            compiler_params=pltpu.CompilerParams(collective_id=0, has_side_effects=True),
        )(block_counts, block_lists, particle_fields, *by_block)

    placed = (
        P(None, AXES),
        P(AXES),
        P(AXES),
        P(AXES),
        P(AXES, None),
        P(AXES, None),
    )
    return jax.shard_map(
        per_device,
        mesh=mesh,
        in_specs=placed,
        out_specs=P(None, AXES),
        check_vma=False,
    )
```

```python
import functools

import jax
import jax.numpy as jnp
from jax import lax
from jax.experimental import pallas as pl
from jax.experimental.pallas import tpu as pltpu
from jax.sharding import PartitionSpec as P

CELLS = 512
CAP_X = 6
CAP_Z = 6
CAP_Y = 12
LANES = 128
HALF = 256
GROUP = 8
GONE = 16
AXES = ("gx", "gy", "gz")


def plan(sizes):
    steps_z = (1,) if sizes["gz"] == 2 else (-1, 1)
    classes = [{}, {"gy": -1}, {"gy": 1}]
    for dz in steps_z:
        classes += [{"gz": dz}, {"gz": dz, "gy": -1}, {"gz": dz, "gy": 1}]
    return steps_z, classes


def migrate_kernel(
    sizes,
    counts_hbm,
    lists_hbm,
    fields_hbm,
    step_hbm,
    live_hbm,
    cell_hbm,
    out_ref,
    bodies,
    ends,
    step,
    live,
    cell,
    offsets,
    offsets_x,
    offsets_slot,
    acc_kept,
    acc,
    alone,
    sent_x,
    got_x,
    sent_meta,
    got_meta,
    sent,
    got,
    counts,
    lists,
    lists_row,
    load_sem,
    send_x_sem,
    recv_x_sem,
    send_meta_sem,
    recv_meta_sem,
    send_sem,
    recv_sem,
    ready,
):
    steps_z, classes = plan(sizes)
    field_count = fields_hbm.shape[0]
    rows = (field_count + 1 + 7) // 8 * 8
    whole = field_count // 8 * 8
    tail = field_count - whole
    blocks = step.shape[0]
    halves = CELLS // HALF
    start_z, start_y = 2 * CAP_X, 2 * CAP_X + 2 * CAP_Z

    me = {axis: lax.axis_index(axis) for axis in AXES}

    def target(moves):
        return {a: lax.rem(me[a] + sizes[a] + d, sizes[a]) for a, d in moves.items()}

    def remote(src, dst, send, recv, moves):
        return pltpu.make_async_remote_copy(
            src_ref=src,
            dst_ref=dst,
            send_sem=send,
            recv_sem=recv,
            device_id=target(moves),
            device_id_type=pl.DeviceIdType.MESH,
        )

    loads = [
        pltpu.make_async_copy(src, dst, load_sem.at[i])
        for i, (src, dst) in enumerate(
            [
                (counts_hbm, counts),
                (lists_hbm, lists),
                (lists_hbm, lists_row),
                (step_hbm, step),
                (live_hbm, live),
                (fields_hbm.at[pl.ds(0, whole)], bodies),
                (cell_hbm, cell),
                (fields_hbm.at[pl.ds(whole, tail)], ends),
            ]
        )
    ]
    for load in loads:
        load.start()

    near = lax.rem(me["gx"], 2)
    far = 1 - near
    moves_x = ({"gx": -1}, {"gx": 1})
    partners = {0: [], -1: [], 1: []}
    seen = set()
    for moves in list(moves_x) + classes[1:]:
        place = tuple(moves.get(a, 0) % sizes[a] for a in AXES)
        if place not in seen:
            seen.add(place)
            partners[moves.get("gy", 0) if sizes["gy"] > 2 else 0].append(moves)
    greets = {-1: me["gy"] == 0, 1: me["gy"] < sizes["gy"] - 1}
    barrier = pltpu.get_barrier_semaphore()

    def signal(semaphore, group):
        for moves in group:
            pl.semaphore_signal(
                semaphore, inc=1, device_id=target(moves), device_id_type=pl.DeviceIdType.MESH
            )

    signal(barrier, partners[0])
    for dy in (-1, 1):
        pl.when(greets[dy])(functools.partial(signal, barrier, partners[dy]))

    expected = len(partners[0])
    for dy in (-1, 1):
        expected += jnp.logical_not(greets[dy]).astype(jnp.int32) * len(partners[dy])

    for load in loads[:3]:
        load.wait()

    lane = lax.broadcasted_iota(jnp.int32, lists_row.shape, 1)
    z_number = blocks + 2 * CAP_X + jnp.where(
        lane < start_z + CAP_Z, lane - start_z + CAP_Z, lane - start_z - CAP_Z
    )
    onward = jnp.zeros(lists_row.shape, jnp.float32)
    for k in range(2 * CAP_Y):
        side, i = k // CAP_Y, k % CAP_Y
        count = jnp.full(lists_row.shape, counts[0, 4 + side])
        hit = (z_number == lists[0, start_y + k]) & (count > i)
        onward = jnp.where(hit, float(1 + side), onward)
    sent_meta[...] = jnp.broadcast_to(onward, sent_meta.shape)

    pl.semaphore_wait(barrier, expected)

    copies_meta = [
        remote(
            sent_meta, got_meta.at[i], send_meta_sem.at[i], recv_meta_sem.at[i], {"gz": dz}
        )
        for i, dz in enumerate(steps_z)
    ]
    for copy in copies_meta:
        copy.start()
    for dy in (-1, 1):
        heard = ready.at[(1 - dy) // 2]
        pl.when(jnp.logical_not(greets[dy]))(functools.partial(signal, heard, partners[dy]))

    first_row = lax.broadcasted_iota(jnp.int32, (8, LANES), 0)

    def columns(e):
        return pl.ds(e * LANES, LANES)

    def alive(e):
        return live[pl.ds(e, 1), :].astype(jnp.float32)

    def own_body(e):
        v = bodies[:, columns(e)]
        top = v[:8]
        top = top + jnp.where(first_row < 3, step[pl.ds(e, 1), :] * pltpu.roll(top, 5, 0), 0.0)
        return jnp.concatenate([top, v[8:]], axis=0) * alive(e)

    def own_end(e):
        return ends[:, columns(e)] * alive(e), cell[pl.ds(e, 1), :].astype(jnp.float32)

    def own_block(e):
        end, where_to = own_end(e)
        return jnp.concatenate([own_body(e), end, end], axis=0), where_to

    def leaving(slot):
        side, i = slot // CAP_X, slot % CAP_X
        return side, i, jnp.minimum(lists[0, slot], blocks - 1), counts[0, side]

    def copies_of(first, count):
        part = pl.ds(first, count)
        return [
            remote(
                sent_x.at[s, part],
                got_x.at[s, part],
                send_x_sem,
                recv_x_sem.at[s],
                {"gx": 2 * s - 1},
            )
            for s in (near, far)
        ]

    body_rows = CAP_X * whole
    copies_x = copies_of(0, body_rows) + copies_of(body_rows, sent_x.shape[1] - body_rows)
    for load in loads[3:6]:
        load.wait()
    for slot in range(2 * CAP_X):
        side, i, e, count = leaving(slot)
        block = jnp.where(jnp.full((whole, LANES), count) > i, own_body(e), 0.0)
        sent_x[side, pl.ds(i * whole, whole), :] = block
    for copy in copies_x[:2]:
        copy.start()
    for load in loads[6:]:
        load.wait()
    for slot in range(2 * CAP_X):
        side, i, e, count = leaving(slot)
        end, where_to = own_end(e)
        taken = jnp.full((tail, LANES), count) > i
        sent_x[side, pl.ds(body_rows + i * tail, tail), :] = jnp.where(taken, end, 0.0)
        where_to = jnp.where(taken[:1], where_to, 0.0)
        sent_x[side, pl.ds(CAP_X * field_count + i, 1), :] = where_to
    for copy in copies_x[2:]:
        copy.start()

    spans = (CAP_X, CAP_X, CAP_Z, CAP_Z, CAP_Y, CAP_Y)
    limit = jnp.zeros(lists_row.shape, jnp.int32)
    away = jnp.zeros(lists_row.shape, jnp.float32)
    start = 0
    for k, span in enumerate(spans):
        here = lane >= start
        limit = jnp.where(here, counts[0, k] + start, limit)
        away = jnp.where(here, float(GONE if k < 4 else k - 3), away)
        start += span
    valid = lane < limit
    entries = lists_row[...]
    own_entry = valid & (entries < blocks)

    def table(ref, first, value, by_lane):
        number = first + lax.broadcasted_iota(jnp.int32, (ref.shape[0], lists_row.shape[1]), 0)
        hit = (lane if by_lane else entries) == number
        total = jnp.sum(jnp.where(hit, value, 0.0), axis=1, keepdims=True)
        ref[...] = jnp.broadcast_to(total, ref.shape)

    table(offsets, 0, jnp.where(valid, away, 0.0), False)
    y_slots = offsets_slot.at[pl.ds(2 * CAP_Z, 2 * CAP_Y)]
    table(y_slots, start_y, jnp.where(own_entry, away, float(GONE)), True)

    pack = 2 * 8
    bf16 = jnp.bfloat16
    row16 = lax.broadcasted_iota(jnp.int32, (pack, LANES), 0)
    code = row16.astype(jnp.float32)
    second = jnp.where(row16 >= 8, 1.0, 0.0)

    zero = jnp.zeros((pack, LANES), bf16)
    one = jnp.ones((pack, LANES), bf16)

    def prepared(v, cells):
        body, end = v[:whole], v[whole:]
        high = body.astype(bf16)
        low = (body - high.astype(jnp.float32)).astype(bf16)
        end_high = end.astype(bf16).astype(jnp.float32)
        end = jnp.where(first_row < tail, end_high, end - end_high)
        end = jnp.concatenate([end, end], axis=0).astype(bf16)
        part = jnp.floor(cells * (1.0 / HALF))
        ahead = (jnp.broadcast_to(cells - part * HALF, (pack, LANES)) - code).astype(bf16)
        right = [
            jnp.where(ahead == jnp.full((pack, LANES), k, bf16), one, zero)
            for k in range(0, HALF, pack)
        ]
        return high, low, end, part, jnp.concatenate(right, axis=0)

    def level(number):
        return jnp.full((pack, LANES), number, jnp.float32).astype(bf16)

    def masked(block, kind, group):
        high, low, end, part, right = block
        part = jnp.broadcast_to(part + kind * halves, (pack, LANES))
        part_end = (part - second).astype(bf16)
        part = part.astype(bf16)
        left = []
        for c in group:
            for h in range(halves):
                here = part == level(c * halves + h)
                left += [jnp.where(here, high, zero), jnp.where(here, low, zero)]
            here = part_end == level(c * halves)
            left.append(jnp.where(here, end, zero))
        return jnp.concatenate(left, axis=0), right

    each = 2 * whole * halves + pack

    def span_of(group):
        return pl.ds((group[0] - 1) * each, len(group) * each)

    def product(pairs):
        left = jnp.concatenate([a for a, _ in pairs], axis=1)
        right = jnp.concatenate([b for _, b in pairs], axis=1)
        return lax.dot_general(
            left, right, (((1,), (1,)), ((), ())), preferred_element_type=jnp.float32
        )

    top_rows = lax.broadcasted_iota(jnp.int32, (8, HALF), 0) < tail

    def packed(r):
        out = []
        for h in range(halves):
            high = 2 * h * whole
            out.append(r[high : high + whole] + r[high + whole : high + 2 * whole])
        ends = [r[2 * halves * whole + 8 * h :][:8] for h in range(halves)]
        ends = [e + pltpu.roll(e, tail, 0) for e in ends]
        return out + [jnp.where(top_rows, ends[0], ends[1])]

    def spread(blocks, kinds, group):
        half = len(blocks) // 2
        minus = [(-high, -low, -end, *rest) for high, low, end, *rest in blocks[half:]]
        pairs = [masked(v, kind, group) for v, kind in zip(blocks[:half] + minus, kinds)]
        return product(pairs[:half]) - product(pairs[half:])

    def own_slot(k):
        return prepared(*own_block(jnp.minimum(lists[0, start_z + k], blocks - 1)))

    def slot_kind(k):
        return offsets_slot[pl.ds(k, 1), :]

    for side in range(2):
        first = 2 * CAP_Z + side * CAP_Y
        slots = range(first, first + CAP_Y)
        pairs = [masked(own_slot(k), slot_kind(k), (1 + side,)) for k in slots]
        acc[span_of((1 + side,)), :] = product(pairs)

    def unpacked(side, i):
        body = got_x[side, pl.ds(i * whole, whole), :]
        rest = got_x[side, pl.ds(CAP_X * whole + i * tail, tail), :]
        cells = got_x[side, pl.ds(CAP_X * field_count + i, 1), :]
        return jnp.concatenate([body, rest, rest], axis=0), cells

    def wait_x(side):
        pltpu.make_async_remote_copy(
            src_ref=sent_x.at[pl.ds(side, 1)],
            dst_ref=got_x.at[pl.ds(side, 1)],
            send_sem=send_x_sem,
            recv_sem=recv_x_sem.at[side],
            device_id=target(moves_x[0]),
            device_id_type=pl.DeviceIdType.MESH,
        ).wait_recv()

    bound = tuple(range(1, len(classes)))
    y_classes, z_classes = bound[:2], bound[2:]

    def got_kind(ref, side, i):
        base = (1 - side) * CAP_X
        return ref[pl.ds(base + i, 1), :]

    def block_sums(ref, i, block):
        plain = masked(block, jnp.zeros((1, LANES), jnp.float32), (0,))
        ref[i] = jnp.concatenate(packed(product([plain])), axis=0)

    for k in range(2 * CAP_Z):
        block_sums(alone, k, own_slot(k))
    wait_x(near)
    near_blocks = [prepared(*unpacked(near, i)) for i in range(CAP_X)]
    for i, block in enumerate(near_blocks):
        block_sums(alone, 2 * CAP_Z + i, block)
    kinds = [got_kind(offsets.at[pl.ds(blocks, 2 * CAP_X)], near, i) for i in range(CAP_X)]
    more = spread(near_blocks, kinds, y_classes)
    for c in y_classes:
        total = acc[span_of((c,)), :] + more[(c - 1) * each : c * each]
        sent[c - 1] = jnp.concatenate(packed(total), axis=0)

    for copy in copies_meta:
        copy.wait_recv()
    if len(steps_z) == 1:
        kind = got_meta[0, :1, :]
    else:
        kind = jnp.where(lane < start_z + CAP_Z, got_meta[1, :1, :], got_meta[0, :1, :] + 3.0)
    in_z = (lane >= start_z) & (lane < start_y)
    away = jnp.where(in_z, kind + 3.0, away)
    table(offsets_x, blocks, jnp.where(valid, away, 0.0), False)
    z_slots = offsets_slot.at[pl.ds(0, 2 * CAP_Z)]
    table(z_slots, start_z, jnp.where(own_entry, away, float(GONE)), True)

    kinds = [slot_kind(k) for k in range(2 * CAP_Z)]
    kinds += [got_kind(offsets_x, near, i) for i in range(CAP_X)]
    kinds = [jnp.concatenate([kind] * (HALF // LANES), axis=1) for kind in kinds]
    for c in z_classes:
        sent[c - 1] = sum(
            jnp.where(kind == float(c), alone[k], 0.0) for k, kind in enumerate(kinds)
        )

    acc_kept[...] = jnp.zeros_like(acc_kept)

    def bin_own(g, carry):
        numbers = [g * GROUP + i for i in range(GROUP)]
        kinds = [offsets[pl.ds(b, 1), :] for b in numbers]
        acc_kept[...] += spread([prepared(*own_block(b)) for b in numbers], kinds, (0,))
        return carry

    wait_x(far)
    far_blocks = [prepared(*unpacked(far, i)) for i in range(CAP_X)]

    def finish(group):
        sums = spread(far_blocks, [got_kind(offsets_x, far, i) for i in range(CAP_X)], group)
        for g, c in enumerate(group):
            pieces = packed(sums[g * each : (g + 1) * each])
            sent[c - 1] += jnp.concatenate(pieces, axis=0)

    def message(c, moves):
        return remote(sent.at[c - 1], got.at[c - 1], send_sem, recv_sem, moves)

    side = jnp.where(me["gy"] == sizes["gy"] - 1, 1, 0)
    along, across = (1, {}), [(3 * q + 4, {"gz": dz}) for q, dz in enumerate(steps_z)]
    straight = [(3 * q + 3, {"gz": dz}) for q, dz in enumerate(steps_z)]
    if len(steps_z) == 1:
        lead = jnp.where(me["gz"] == 0, 0, 1)
        ahead = [(1 + 3 * lead, {"gz": lead})]
        behind = [(4 - 3 * lead, {"gz": 1 - lead})]
    else:
        ahead, behind = across, [along]

    def on_side(group, s):
        return [message(c + s, moves | {"gy": 2 * s - 1}) for c, moves in group]

    finish([c + side for c, _ in ahead])
    for dy in (-1, 1):
        heard = functools.partial(pl.semaphore_wait, ready.at[(1 + dy) // 2], len(partners[dy]))
        if partners[dy]:
            pl.when(greets[dy])(heard)
    first = on_side(ahead, side)
    held = jnp.where(near == 1, 1, 0)
    lax.fori_loop(0, held, bin_own, 0)
    for copy in first:
        copy.start()
    finish([c + s for c, _ in behind for s in (0, 1)] + [c + 1 - side for c, _ in ahead] + [c for c, _ in straight])
    rest = on_side(behind, side)
    for copy in rest:
        copy.start()
    later = held + 2
    lax.fori_loop(held, later, bin_own, 0)
    direct = on_side(ahead, 1 - side) + on_side(behind, 1 - side)
    direct += [message(c, moves) for c, moves in straight]
    for copy in direct:
        copy.start()
    rest += direct
    copies = first + rest

    for side in range(2):
        pairs = []
        for i in range(CAP_X):
            pairs.append(masked(prepared(*unpacked(side, i)), got_kind(offsets_x, side, i), (0,)))
        acc_kept[...] += product(pairs)

    lax.fori_loop(later, blocks // GROUP, bin_own, 0)

    total = jnp.concatenate(packed(acc_kept[...]), axis=0)
    remote(sent_x, got_x, send_x_sem, recv_x_sem.at[0], moves_x[0]).wait_send()
    for copy in copies_meta:
        copy.wait_send()
    everything = remote(sent, got, send_sem, recv_sem, classes[1])
    everything.wait_send()
    everything.wait_recv()
    for c in bound:
        total = total + got[c - 1]
    for h in range(halves):
        here = pl.ds(h * HALF, HALF)
        out_ref[:whole, here] = total[h * whole : (h + 1) * whole]
        last = halves * whole + h * tail
        out_ref[whole:, here] = total[last : last + tail]


def solution(mesh):
    sizes = {axis: mesh.shape[axis] for axis in AXES}

    def per_device(particle_fields, step_length, live_mask, dest_cell, block_counts, block_lists):
        field_count, particles = particle_fields.shape
        blocks = particles // LANES
        rows = (field_count + 1 + 7) // 8 * 8
        steps_z, classes = plan(sizes)
        sends = len(classes) - 1
        halves = CELLS // HALF
        sum_rows = (field_count * halves + 7) // 8 * 8
        packed_x = (CAP_X * (field_count + 1) + 7) // 8 * 8
        slots = 2 * CAP_Z + 2 * CAP_Y
        each = 2 * (field_count // 8 * 8) * halves + 16

        by_block = [a.reshape(blocks, LANES) for a in (step_length, live_mask, dest_cell)]
        any_space = pl.BlockSpec(memory_space=pl.ANY)
        f32 = jnp.float32
        return pl.pallas_call(
            functools.partial(migrate_kernel, sizes),
            out_shape=pltpu.VMEM((field_count, CELLS), f32),
            in_specs=[any_space] * 6,
            out_specs=pl.BlockSpec(memory_space=pltpu.VMEM),
            scratch_shapes=[
                pltpu.VMEM((field_count // 8 * 8, particles), f32),
                pltpu.VMEM((field_count % 8, particles), f32),
                pltpu.VMEM((blocks, LANES), f32),
                pltpu.VMEM((blocks, LANES), jnp.int32),
                pltpu.VMEM((blocks, LANES), jnp.int32),
                pltpu.VMEM((blocks + (2 * CAP_X + 7) // 8 * 8, LANES), f32),
                pltpu.VMEM(((2 * CAP_X + 7) // 8 * 8, LANES), f32),
                pltpu.VMEM(((slots + 7) // 8 * 8, LANES), f32),
                pltpu.VMEM((each, HALF), f32),
                pltpu.VMEM((each * 2, HALF), f32),
                pltpu.VMEM((2 * CAP_Z + CAP_X, sum_rows, HALF), f32),
                pltpu.VMEM((2, packed_x, LANES), f32),
                pltpu.VMEM((2, packed_x, LANES), f32),
                pltpu.VMEM((8, block_lists.shape[1]), f32),
                pltpu.VMEM((len(steps_z), 8, block_lists.shape[1]), f32),
                pltpu.VMEM((sends, sum_rows, HALF), f32),
                pltpu.VMEM((sends, sum_rows, HALF), f32),
                pltpu.SMEM(block_counts.shape, jnp.int32),
                pltpu.SMEM(block_lists.shape, jnp.int32),
                pltpu.VMEM(block_lists.shape, jnp.int32),
                pltpu.SemaphoreType.DMA((8,)),
                pltpu.SemaphoreType.DMA,
                pltpu.SemaphoreType.DMA((2,)),
                pltpu.SemaphoreType.DMA((len(steps_z),)),
                pltpu.SemaphoreType.DMA((len(steps_z),)),
                pltpu.SemaphoreType.DMA,
                pltpu.SemaphoreType.DMA,
                pltpu.SemaphoreType.REGULAR((2,)),
            ],
            compiler_params=pltpu.CompilerParams(collective_id=0, has_side_effects=True),
        )(block_counts, block_lists, particle_fields, *by_block)

    placed = (
        P(None, AXES),
        P(AXES),
        P(AXES),
        P(AXES),
        P(AXES, None),
        P(AXES, None),
    )
    return jax.shard_map(
        per_device,
        mesh=mesh,
        in_specs=placed,
        out_specs=P(None, AXES),
        check_vma=False,
    )
```
